256 devices in a mesh: row: 32 (over z, x_lo, core), col: 8 (over x_hi, y).
Axes of the slice: x: 4 (x_hi: 2, x_lo: 2; x = x_hi * 2 + x_lo), y: 4, z: 8, core: 2. Of those that a mesh axis runs over, the one named last changes fastest.
Arguments:
- pair_map: float32 [512, 512, 128], P('row', 'col'), may hold values from -6 to 6
- pair_mask: int32 [512, 512], P('row', 'col'), may hold values 0 or 1
- in_gain: float32 [128], replicated, may hold values from 0.25 to 1.75
- in_bias: float32 [128], replicated, may hold values from -3 to 3
- w_proj: bfloat16 [128, 512], replicated, may hold values from -0.5 to 0.5
- w_gate: bfloat16 [128, 128], replicated, may hold values from -0.5 to 0.5
- out_gain: float32 [128], replicated, may hold values from 0.25 to 1.75
- out_bias: float32 [128], replicated, may hold values from -3 to 3
- w_out: bfloat16 [128, 128], replicated, may hold values from -0.5 to 0.5
Outputs:
- update: float32 [512, 512, 128], P('row', 'col')
The draws below stay inside these ranges and needn't reach their ends.
All inputs are finite; a program needn't handle non-finite values. No bound on the sum of `pair_mask` on one device may be relied on, other than what follows from the above.
Results may differ from the reference program's by a relative error of at most 0.0035.
Values may be sent and summed in bfloat16 or wider, within the bound.
A program may use at most 128 MiB of HBM per device.

```python
import jax
import jax.numpy as jnp
from jax import lax

C = 128
CH = 128
NRES = 512


def place_ends(drawn, key, least, top_value):
    shape = drawn.shape
    index_at = [jax.random.randint(jax.random.fold_in(key, axis), (), 0, shape[axis]) for axis in range(len(shape))]
    drawn = drawn.at[tuple(index_at)].set(least)
    longest = shape.index(max(shape))
    index_at[longest] = (index_at[longest] + 1) % shape[longest]
    return drawn.at[tuple(index_at)].set(top_value)


def block_levels(own_key, dims, shards, low, top_value):
    level = 1.0
    for axis_at, parts in shards:
        draws = jax.random.uniform(jax.random.fold_in(jax.random.fold_in(own_key, 6), axis_at), (parts,), jnp.float32, low / len(shards), top_value / len(shards))
        level = level * jnp.repeat(jnp.exp(draws), dims[axis_at] // parts).reshape((-1,) + (1,) * (len(dims) - 1 - axis_at))
    return level


def noise(own_key, extent, deviation, reach, pieces=(), held_as=jnp.bfloat16):
    loudness = block_levels(own_key, extent, pieces, -0.22, 0.18) if pieces else 1.0
    entries = jax.random.normal(own_key, extent, jnp.float32) * deviation * loudness
    return jnp.minimum(jnp.maximum(entries, -reach), reach).astype(held_as)


def setup_inputs(seed: int = 0) -> dict:
    streams_of = jax.random.split(jax.random.key(seed), 10)
    return {
        "pair_map": noise(streams_of[0], (NRES, NRES, C), 1.0, 6.0, ((0, 32), (1, 8)), jnp.float32),
        "pair_mask": place_ends((jax.random.randint(streams_of[1], (NRES, NRES), 0, 4) < 3).astype(jnp.int32), jax.random.fold_in(streams_of[1], 1), 0, 1),
        "in_gain": jnp.clip(1.0 + 0.15 * jax.random.normal(streams_of[2], (C,), jnp.float32), 0.25, 1.75),
        "in_bias": noise(streams_of[3], (C,), 0.5, 3.0, (), jnp.float32),
        "w_proj": noise(streams_of[4], (C, 4 * CH), C ** -0.5, 0.5),
        "w_gate": noise(streams_of[5], (C, C), C ** -0.5, 0.5),
        "out_gain": jnp.clip(1.0 + 0.15 * jax.random.normal(streams_of[6], (CH,), jnp.float32), 0.25, 1.75),
        "out_bias": noise(streams_of[7], (CH,), 0.5, 3.0, (), jnp.float32),
        "w_out": noise(streams_of[8], (CH, C), CH ** -0.5, 0.5),
    }


def layer_norm(values, gain, bias):
    average = lax.optimization_barrier(jnp.mean(values, axis=-1, keepdims=True))
    variance = lax.optimization_barrier(jnp.mean(jnp.square(values - average), axis=-1, keepdims=True))
    return (values - average) * lax.rsqrt(variance + 1e-05) * gain + bias

def reference(pair_map, pair_mask, in_gain, in_bias, w_proj, w_gate, out_gain, out_bias, w_out):
    normed = layer_norm(pair_map, in_gain, in_bias).astype(jnp.bfloat16)
    flattened = normed.reshape(-1, C)
    projected = jnp.dot(flattened, w_proj, preferred_element_type=jnp.float32).reshape(NRES, NRES, 4 * CH)
    masked = pair_mask.astype(jnp.float32)[..., None]
    left_side = (masked * jax.nn.sigmoid(projected[..., :CH]) * projected[..., CH:2 * CH]).astype(jnp.bfloat16)
    right_side = (masked * jax.nn.sigmoid(projected[..., 2 * CH:3 * CH]) * projected[..., 3 * CH:]).astype(jnp.bfloat16)
    gating = jax.nn.sigmoid(jnp.dot(flattened, w_gate, preferred_element_type=jnp.float32)).reshape(NRES, NRES, C)
    summed = jnp.einsum('ikc,jkc->ijc', left_side.astype(jnp.float32), right_side.astype(jnp.float32), precision=lax.Precision.HIGHEST)
    normed_sum = layer_norm(summed, out_gain, out_bias).astype(jnp.bfloat16)
    result = jnp.dot(normed_sum.reshape(-1, CH), w_out, preferred_element_type=jnp.float32).reshape(NRES, NRES, C)
    return gating * result
```

```python
import jax
import jax.numpy as jnp
from jax import lax
from jax.experimental import pallas as pl
from jax.experimental.pallas import tpu as pltpu
from jax.sharding import PartitionSpec as P

MESH = pl.DeviceIdType.MESH
PLANES = 8
QUAD = 4
PEERS = 32
HELD = 4
PITCH = 136
NT = (((1,), (1,)), ((), ()))
TN = (((0,), (0,)), ((), ()))


def dot(a, b, dims):
    return lax.dot_general(a, b, dims, preferred_element_type=jnp.float32)


def halves(a, b):
    low = lax.broadcasted_iota(jnp.int32, a.shape, 1) < 64
    return jnp.where(low, a, pltpu.roll(b, 64, 1)), jnp.where(low, pltpu.roll(a, 64, 1), b)


def kernel(
    x_ref, mask_ref, in_gain, in_bias, w_proj, w_gate, out_gain, out_bias, w_out, out_ref,
    stage, normed, gate, send_r, send_l, recv_r, recv_l, left, right, s_send, s_recv,
    send_r_sem, recv_r_sem, send_l_sem, recv_l_sem, up_s, up_r, down_s, down_r, s_s, s_r,
):
    row, col = lax.axis_index("row"), lax.axis_index("col")
    z, quarter = lax.div(row, QUAD), lax.rem(row, QUAD)
    me = col * QUAD + quarter
    above = {"row": lax.rem(row + QUAD, PLANES * QUAD), "col": col}
    below = {"row": lax.rem(row + (PLANES - 1) * QUAD, PLANES * QUAD), "col": col}

    def peer(other):
        return {"row": z * QUAD + lax.rem(other, QUAD), "col": lax.div(other, QUAD)}

    def others(step):
        def run(o, carry):
            step(lax.rem(me + o, PEERS))
            return carry

        lax.fori_loop(1, PEERS, run, 0)

    barrier = pltpu.get_barrier_semaphore()
    others(lambda o: pl.semaphore_signal(barrier, inc=1, device_id=peer(o), device_id_type=MESH))
    for neighbour in (above, below):
        pl.semaphore_signal(barrier, inc=1, device_id=neighbour, device_id_type=MESH)

    lane_low = lax.broadcasted_iota(jnp.int32, (8, 128), 1) < 64
    mask = mask_ref[...].astype(jnp.float32)
    masked = jnp.concatenate([mask[:8], mask[8:]], axis=1)
    weights = jnp.transpose(w_proj[...].astype(jnp.float32)).astype(jnp.bfloat16)

    def layer_norm_in(t):
        v = jnp.concatenate([x_ref[t], x_ref[t + 8]], axis=0)
        average = jnp.mean(v, axis=1, keepdims=True)
        variance = jnp.mean(jnp.square(v - average), axis=1, keepdims=True)
        return ((v - average) * lax.rsqrt(variance + 1e-05) * in_gain[...] + in_bias[...]).astype(jnp.bfloat16)

    def project(t, first):
        p = dot(weights[first : first + 256], normed[t], NT)
        side = masked[t : t + 1] * jax.nn.sigmoid(p[:128]) * p[128:]
        stage[pl.ds(t * PITCH, 128), :] = side

    def pack(send):
        for g in range(64):
            pair = [stage[pl.ds(2 * g + e, 8, stride=PITCH), :] for e in range(2)]
            send[g // 2, g % 2] = jnp.concatenate(pair, axis=0).astype(jnp.bfloat16)

    def hand_over(send, recv, send_sem, recv_sem, other):
        return pltpu.make_async_remote_copy(
            src_ref=send.at[other], dst_ref=recv.at[me], send_sem=send_sem.at[other], recv_sem=recv_sem.at[me],
            device_id=peer(other), device_id_type=MESH,
        )

    def arrival(recv, send_sem, recv_sem, other):
        return pltpu.make_async_remote_copy(
            src_ref=recv.at[other], dst_ref=recv.at[other], send_sem=send_sem.at[other], recv_sem=recv_sem.at[other],
            device_id=peer(other), device_id_type=MESH,
        )

    def regroup(recv, store):
        for g in range(2):
            for kp in range(4):
                for rr in range(QUAD):
                    a = recv[8 * kp + rr, g].astype(jnp.float32)
                    b = recv[8 * kp + 4 + rr, g].astype(jnp.float32)
                    first, second = halves(a, b)
                    for e in range(2):
                        rows = slice(8 * e, 8 * e + 8)
                        tile = jnp.concatenate([first[rows], second[rows]], axis=0).astype(jnp.bfloat16)
                        store(2 * g + e, slice(16 * rr, 16 * rr + 16), slice(128 * kp, 128 * kp + 128), tile)

    for t in range(8):
        normed[t] = layer_norm_in(t)
        project(t, 256)
    pack(send_r)
    pl.semaphore_wait(barrier, PEERS - 1 + 2)
    others(lambda o: hand_over(send_r, recv_r, send_r_sem, recv_r_sem, o).start())
    recv_r[me] = send_r[me]

    for t in range(8):
        project(t, 0)
    pack(send_l)
    others(lambda o: hand_over(send_l, recv_l, send_l_sem, recv_l_sem, o).start())
    recv_l[me] = send_l[me]

    others(lambda o: arrival(recv_r, send_r_sem, recv_r_sem, o).wait_recv())

    def store_right(ch, rows, lanes, tile):
        right[z, ch, rows, lanes] = tile

    def up(d, ch):
        block = lax.rem(z + PLANES - d + 1, PLANES)
        return pltpu.make_async_remote_copy(
            src_ref=right.at[block, ch], dst_ref=right.at[block, ch], send_sem=up_s.at[d - 1, ch],
            recv_sem=up_r.at[d - 1, ch], device_id=above, device_id_type=MESH,
        )

    def down(d, ch):
        block = lax.rem(z + d - 1, PLANES)
        return pltpu.make_async_remote_copy(
            src_ref=right.at[block, ch], dst_ref=right.at[block, ch], send_sem=down_s.at[d - 1, ch],
            recv_sem=down_r.at[d - 1, ch], device_id=below, device_id_type=MESH,
        )

    regroup(recv_r, store_right)
    for ch in range(HELD):
        up(1, ch).start()
        down(1, ch).start()

    for t in range(8):
        p = jax.nn.sigmoid(dot(normed[t], w_gate[...], (((1,), (0,)), ((), ()))))
        gate[t] = p[:64]
        gate[t + 8] = p[64:]

    others(lambda o: arrival(recv_l, send_l_sem, recv_l_sem, o).wait_recv())

    def store_left(ch, rows, lanes, tile):
        left[ch, rows, lanes] = tile

    regroup(recv_l, store_left)

    def s_copy(block, rr, first, count):
        return pltpu.make_async_remote_copy(
            src_ref=s_send.at[block, rr, pl.ds(first, count)],
            dst_ref=s_recv.at[pl.ds(pl.multiple_of(me * 32 + first, 8), count)],
            send_sem=s_s.at[block, rr], recv_sem=s_r.at[me],
            device_id={"row": z * QUAD + rr, "col": block}, device_id_type=MESH,
        )

    def s_block(block, ch):
        r = right[block, ch]
        s = dot(left[ch], jnp.concatenate([r, r], axis=0), NT)
        for rr in range(QUAD):
            tile = jnp.where(lane_low, s[16 * rr : 16 * rr + 8], s[16 * rr + 8 : 16 * rr + 16])
            mine = jnp.logical_and(block == col, quarter == rr)

            @pl.when(mine)
            def _():
                s_recv[pl.ds(pl.multiple_of(me * 32 + ch * 8, 8), 8), :] = tile

            @pl.when(jnp.logical_not(mine))
            def _():
                s_send[block, rr, pl.ds(pl.multiple_of(ch * 8, 8), 8), :] = tile
                s_copy(block, rr, pl.multiple_of(ch * 8, 8), 8).start()

    def own(ch, carry):
        s_block(z, ch)
        return carry

    lax.fori_loop(0, HELD, own, 0)

    def ring(n, carry):
        d, ch = lax.div(n, HELD) + 1, lax.rem(n, HELD)
        up(d, ch).wait_recv()

        @pl.when(jnp.logical_or(d < 3, ch < 2))
        def _():
            up(d + 1, ch).start()

        down(d, ch).wait_recv()

        @pl.when(jnp.logical_or(d < 3, ch >= 2))
        def _():
            down(d + 1, ch).start()

        s_block(lax.rem(z + PLANES - d, PLANES), ch)
        s_block(lax.rem(z + d, PLANES), ch)
        return carry

    lax.fori_loop(0, 3 * HELD, ring, 0)
    for ch in range(2):
        up(4, ch).wait_recv()
        s_block(lax.rem(z + 4, PLANES), ch)
        down(4, ch + 2).wait_recv()
        s_block(lax.rem(z + 4, PLANES), ch + 2)

    gain = jnp.transpose(jnp.broadcast_to(out_gain[...], (128, 128)))
    bias = jnp.transpose(jnp.broadcast_to(out_bias[...], (128, 128)))

    def s_arrival(o):
        rows = pl.ds(pl.multiple_of(o * 32, 8), 32)
        pltpu.make_async_remote_copy(
            src_ref=s_recv.at[rows], dst_ref=s_recv.at[rows], send_sem=s_s.at[0, 0], recv_sem=s_r.at[o],
            device_id=peer(o), device_id_type=MESH,
        ).wait_recv()

    others(s_arrival)
    for t in range(8):
        v = s_recv[pl.ds(t, 128, stride=8), :]
        average = jnp.mean(v, axis=0, keepdims=True)
        variance = jnp.mean(jnp.square(v - average), axis=0, keepdims=True)
        n = ((v - average) * lax.rsqrt(variance + 1e-05) * gain + bias).astype(jnp.bfloat16)
        y = dot(n, w_out[...], TN)
        out_ref[t] = gate[t] * y[:64]
        out_ref[t + 8] = gate[t + 8] * y[64:]

    def sent(o):
        hand_over(send_r, recv_r, send_r_sem, recv_r_sem, o).wait_send()
        hand_over(send_l, recv_l, send_l_sem, recv_l_sem, o).wait_send()
        s_copy(lax.div(o, QUAD), lax.rem(o, QUAD), 0, 32).wait_send()

    others(sent)

    def ring_sent(n, carry):
        d, ch = lax.div(n, HELD) + 1, lax.rem(n, HELD)
        up(d, ch).wait_send()
        down(d, ch).wait_send()
        return carry

    lax.fori_loop(0, 3 * HELD, ring_sent, 0)
    for ch in range(2):
        up(4, ch).wait_send()
        down(4, ch + 2).wait_send()


def local(pair_map, pair_mask, in_gain, in_bias, w_proj, w_gate, out_gain, out_bias, w_out):
    f32, bf16 = jnp.float32, jnp.bfloat16
    vmem, dma = pltpu.VMEM, pltpu.SemaphoreType.DMA
    return pl.pallas_call(
        kernel,
        out_shape=jax.ShapeDtypeStruct(pair_map.shape, f32),
        in_specs=[pl.BlockSpec(memory_space=vmem)] * 9,
        out_specs=pl.BlockSpec(memory_space=vmem),
        scratch_shapes=[
            vmem((8 * PITCH, 128), f32),
            vmem((8, 128, 128), bf16),
            vmem((16, 64, 128), f32),
            vmem((PEERS, 2, 16, 128), bf16),
            vmem((PEERS, 2, 16, 128), bf16),
            vmem((PEERS, 2, 16, 128), bf16),
            vmem((PEERS, 2, 16, 128), bf16),
            vmem((HELD, 64, 512), bf16),
            vmem((PLANES, HELD, 64, 512), bf16),
            vmem((PLANES, QUAD, 32, 128), f32),
            vmem((1024, 128), f32),
            dma((PEERS,)), dma((PEERS,)), dma((PEERS,)), dma((PEERS,)),
            dma((4, HELD)), dma((4, HELD)), dma((4, HELD)), dma((4, HELD)),
            dma((PLANES, QUAD)), dma((PEERS,)),
        ],
        compiler_params=pltpu.CompilerParams(collective_id=0, has_side_effects=True),
    )(
        pair_map, pair_mask, in_gain.reshape(1, -1), in_bias.reshape(1, -1), w_proj, w_gate,
        out_gain.reshape(1, -1), out_bias.reshape(1, -1), w_out,
    )


def solution(mesh):
    placed = (P("row", "col", None), P("row", "col"), P(), P(), P(), P(), P(), P(), P())
    return jax.shard_map(local, mesh=mesh, in_specs=placed, out_specs=P("row", "col", None), check_vma=False)
```

```python
import jax
import jax.numpy as jnp
from jax import lax
from jax.experimental import pallas as pl
from jax.experimental.pallas import tpu as pltpu
from jax.sharding import PartitionSpec as P

MESH = pl.DeviceIdType.MESH
PLANES = 8
QUAD = 4
PEERS = 32
HELD = 4
PITCH = 136
NN = (((1,), (0,)), ((), ()))
NT = (((1,), (1,)), ((), ()))
TN = (((0,), (0,)), ((), ()))


def steps(reach):
    every = [(dx, dy, dh) for dx in range(4) for dy in range(4) for dh in range(2) if dx or dy or dh]
    return sorted(every, key=lambda s: reach(min(s[0], 4 - s[0]) + min(s[1], 4 - s[1])))


def dot(a, b, dims):
    return lax.dot_general(a, b, dims, preferred_element_type=jnp.float32)


def halves(a, b):
    low = lax.broadcasted_iota(jnp.int32, a.shape, 1) < 64
    return jnp.where(low, a, pltpu.roll(b, 64, 1)), jnp.where(low, pltpu.roll(a, 64, 1), b)


def kernel(
    x_hbm, mask_hbm, in_gain_hbm, in_bias_hbm, w_proj_hbm, w_gate_hbm, out_gain_hbm, out_bias_hbm, w_out_hbm, out_ref,
    x_ref, mask_ref, in_gain, in_bias, w_proj, w_gate, out_gain, out_bias, w_out, x_sem, in_sem,
    stage, normed, gate, send_r, send_l, recv_r, recv_l, left, right, s_send, s_recv, column,
    send_r_sem, recv_r_sem, send_l_sem, recv_l_sem, up_s, up_r, down_s, down_r, s_s, s_r,
):
    row, col = lax.axis_index("row"), lax.axis_index("col")
    z, quarter = lax.div(row, QUAD), lax.rem(row, QUAD)
    me = col * QUAD + quarter
    x = lax.div(col, 4) * 2 + lax.div(quarter, 2)
    y, core = lax.rem(col, 4), lax.rem(quarter, 2)
    strip = lax.div(col, 2)
    above = {"row": lax.rem(row + QUAD, PLANES * QUAD), "col": col}
    below = {"row": lax.rem(row + (PLANES - 1) * QUAD, PLANES * QUAD), "col": col}

    def peer(other):
        return {"row": z * QUAD + lax.rem(other, QUAD), "col": lax.div(other, QUAD)}

    def each(reach, step):
        for dx, dy, dh in steps(reach):
            to_x, to_y, to_core = lax.rem(x + dx, 4), lax.rem(y + dy, 4), lax.rem(core + dh, 2)
            step(lax.div(to_x, 2) * 16 + to_y * 4 + lax.rem(to_x, 2) * 2 + to_core)

    barrier = pltpu.get_barrier_semaphore()
    each(lambda hops: -hops, lambda o: pl.semaphore_signal(barrier, inc=1, device_id=peer(o), device_id_type=MESH))
    for neighbour in (above, below):
        pl.semaphore_signal(barrier, inc=1, device_id=neighbour, device_id_type=MESH)

    x_in = [
        pltpu.make_async_copy(x_hbm.at[:, pl.ds(2 * n, 2)], x_ref.at[:, pl.ds(2 * n, 2)], x_sem.at[n]) for n in range(4)
    ]
    small = [
        pltpu.make_async_copy(src, dst, in_sem.at[n])
        for n, (src, dst) in enumerate((
            (in_gain_hbm, in_gain), (in_bias_hbm, in_bias), (w_proj_hbm, w_proj), (mask_hbm, mask_ref),
            (w_gate_hbm, w_gate), (out_gain_hbm, out_gain), (out_bias_hbm, out_bias), (w_out_hbm, w_out),
        ))
    ]
    for copy in small[:4] + x_in + small[4:]:
        copy.start()
    for copy in small[:4]:
        copy.wait()

    lane_low = lax.broadcasted_iota(jnp.int32, (8, 128), 1) < 64
    mask = mask_ref[...].astype(jnp.float32)
    masked = jnp.concatenate([mask[:8], mask[8:]], axis=1)
    weights = jnp.transpose(w_proj[...].astype(jnp.float32)).astype(jnp.bfloat16)

    def layer_norm_in(t):
        v = jnp.concatenate([x_ref[0, t], x_ref[1, t]], axis=0)
        average = jnp.mean(v, axis=1, keepdims=True)
        variance = jnp.mean(jnp.square(v - average), axis=1, keepdims=True)
        return ((v - average) * lax.rsqrt(variance + 1e-05) * in_gain[...] + in_bias[...]).astype(jnp.bfloat16)

    def project(t, first):
        p = dot(weights[first : first + 256], normed[t], NT)
        side = masked[t : t + 1] * jax.nn.sigmoid(p[:128]) * p[128:]
        stage[pl.ds(t * PITCH, 128), :] = side

    def pack(send):
        for g in range(64):
            pair = [stage[pl.ds(2 * g + e, 8, stride=PITCH), :] for e in range(2)]
            send[g // 2, g % 2] = jnp.concatenate(pair, axis=0).astype(jnp.bfloat16)

    def move(src, dst, send_sem, recv_sem, to):
        return pltpu.make_async_remote_copy(
            src_ref=src, dst_ref=dst, send_sem=send_sem, recv_sem=recv_sem, device_id=to, device_id_type=MESH
        )

    def regroup(recv, strip, store):
        for g in range(2):
            for rr in range(QUAD):
                a = recv[8 * strip + rr, g].astype(jnp.float32)
                b = recv[8 * strip + 4 + rr, g].astype(jnp.float32)
                first, second = halves(a, b)
                for e in range(2):
                    rows = slice(8 * e, 8 * e + 8)
                    tile = jnp.concatenate([first[rows], second[rows]], axis=0).astype(jnp.bfloat16)
                    store(2 * g + e, slice(16 * rr, 16 * rr + 16), tile)

    for t in range(8):
        if t % 2 == 0:
            x_in[t // 2].wait()
        normed[t] = layer_norm_in(t)
        project(t, 256)
    pack(send_r)
    pl.semaphore_wait(barrier, PEERS - 1 + 2)
    each(
        lambda hops: (1, 2, 3, 4, 0)[hops],
        lambda o: move(send_r.at[o], recv_r.at[me], send_r_sem, recv_r_sem.at[strip], peer(o)).start(),
    )
    recv_r[me] = send_r[me]

    for t in range(8):
        project(t, 0)
    pack(send_l)
    each(
        lambda hops: -hops,
        lambda o: move(send_l.at[o], recv_l.at[me], send_l_sem, recv_l_sem, peer(o)).start(),
    )
    recv_l[me] = send_l[me]

    for copy in small[4:]:
        copy.wait()
    for t in range(8):
        p = jax.nn.sigmoid(dot(normed[t], w_gate[...], NN))
        gate[t] = p[:64]
        gate[t + 8] = p[64:]
    column[0] = jnp.transpose(jnp.broadcast_to(out_gain[...], (128, 128)))
    column[1] = jnp.transpose(jnp.broadcast_to(out_bias[...], (128, 128)))

    def near(e):
        return lax.rem(lax.div(strip, 2) + e // 2, 2) * 2 + lax.rem(strip + e % 2, 2)

    def up(d, e):
        piece = right.at[lax.rem(z + PLANES - d + 1, PLANES) * 4 + near(e)]
        return move(piece, piece, up_s, up_r.at[d - 1, e], above)

    def down(d, e):
        piece = right.at[lax.rem(z + d - 1, PLANES) * 4 + near(e)]
        return move(piece, piece, down_s, down_r.at[d - 1, e], below)

    for e in range(4):
        got = near(e)
        arrived = recv_r.at[pl.ds(8 * got, 8 if e else 7)]
        move(arrived, arrived, send_r_sem, recv_r_sem.at[got], above).wait_recv()

        def store_right(ch, rows, tile, got=got):
            right[z * 4 + got, ch, rows] = tile

        regroup(recv_r, got, store_right)
        up(1, e).start()
        down(1, e).start()

    def store_left(strip):
        def store(ch, rows, tile):
            left[ch, rows, slice(128 * strip, 128 * strip + 128)] = tile

        return store

    def s_block(block, ch):
        r = jnp.concatenate([right[block * 4 + k, ch] for k in range(4)], axis=1)
        s = dot(left[ch], jnp.concatenate([r, r], axis=0), NT)
        for rr in range(QUAD):
            tile = jnp.where(lane_low, s[16 * rr : 16 * rr + 8], s[16 * rr + 8 : 16 * rr + 16])
            mine = jnp.logical_and(block == col, quarter == rr)
            dst = s_recv.at[pl.ds(pl.multiple_of(me * 32 + ch * 8, 8), 8)]

            @pl.when(mine)
            def _():
                dst[...] = tile

            @pl.when(jnp.logical_not(mine))
            def _():
                src = s_send.at[pl.ds(pl.multiple_of((block * QUAD + rr) * 32 + ch * 8, 8), 8)]
                src[...] = tile
                move(src, dst, s_s, s_r, {"row": z * QUAD + rr, "col": block}).start()

    def pair(d, ch):
        s_block(lax.rem(z + PLANES - d, PLANES), ch)
        s_block(lax.rem(z + d, PLANES), ch)

    def forward(d, e):
        up(d, e).wait_recv()
        if d < 3 or e < 2:
            up(d + 1, e).start()
        down(d, e).wait_recv()
        if d < 3 or e >= 2:
            down(d + 1, e).start()

    forward(1, 0)
    forward(1, 1)
    arrived = recv_l.at[pl.ds(0, PEERS - 1)]
    move(arrived, arrived, send_l_sem, recv_l_sem, above).wait_recv()
    for k in range(4):
        regroup(recv_l, k, store_left(k))
    for e in range(2, 4):
        forward(1, e)
        for ch in range(2 * e - 4, 2 * e - 2):
            s_block(z, ch)
    for d in range(2, 4):
        for e in range(4):
            forward(d, e)
            pair(d - 1, e)
    for n in range(2):
        pair(3, 2 * n)
        pair(3, 2 * n + 1)
        up(4, n).wait_recv()
        down(4, n + 2).wait_recv()
    for ch in range(HELD):
        s_block(lax.rem(z + 4, PLANES), ch)

    sent = send_r.at[pl.ds(0, PEERS - 1)]
    move(sent, sent, send_r_sem, recv_r_sem.at[0], above).wait_send()
    move(sent, sent, send_l_sem, recv_l_sem, above).wait_send()
    sent = right.at[pl.ds(0, 14)]
    move(sent, sent, up_s, up_r.at[0, 0], above).wait_send()
    move(sent, sent, down_s, down_r.at[0, 0], below).wait_send()
    sent = s_send.at[pl.ds(0, (PEERS - 1) * 32)]
    move(sent, sent, s_s, s_r, above).wait_send()
    arrived = s_recv.at[pl.ds(0, (PEERS - 1) * 32)]
    move(arrived, arrived, s_s, s_r, above).wait_recv()
    for t in range(8):
        v = s_recv[pl.ds(t, 128, stride=8), :]
        average = jnp.mean(v, axis=0, keepdims=True)
        variance = jnp.mean(jnp.square(v - average), axis=0, keepdims=True)
        n = ((v - average) * lax.rsqrt(variance + 1e-05) * column[0] + column[1]).astype(jnp.bfloat16)
        o = dot(n, w_out[...], TN)
        out_ref[0, t] = gate[t] * o[:64]
        out_ref[1, t] = gate[t + 8] * o[64:]


def local(pair_map, pair_mask, in_gain, in_bias, w_proj, w_gate, out_gain, out_bias, w_out):
    f32, bf16 = jnp.float32, jnp.bfloat16
    vmem, dma = pltpu.VMEM, pltpu.SemaphoreType.DMA
    split = (2, 8, 64, 128)
    args = (
        pair_map.reshape(split), pair_mask, in_gain.reshape(1, -1), in_bias.reshape(1, -1), w_proj, w_gate,
        out_gain.reshape(1, -1), out_bias.reshape(1, -1), w_out,
    )
    out = pl.pallas_call(
        kernel,
        out_shape=jax.ShapeDtypeStruct(split, f32),
        in_specs=[pl.BlockSpec(memory_space=pltpu.HBM)] * 9,
        out_specs=pl.BlockSpec(memory_space=vmem),
        scratch_shapes=[
            *(vmem(a.shape, a.dtype) for a in args),
            dma((4,)), dma((8,)),
            vmem((8 * PITCH, 128), f32),
            vmem((8, 128, 128), bf16),
            vmem((16, 64, 128), f32),
            vmem((PEERS, 2, 16, 128), bf16),
            vmem((PEERS, 2, 16, 128), bf16),
            vmem((PEERS, 2, 16, 128), bf16),
            vmem((PEERS, 2, 16, 128), bf16),
            vmem((HELD, 64, 512), bf16),
            vmem((PLANES * 4, HELD, 64, 128), bf16),
            vmem((1024, 128), f32),
            vmem((1024, 128), f32),
            vmem((2, 128, 128), f32),
            dma, dma((4,)), dma, dma, dma, dma((4, 4)), dma, dma((4, 4)), dma, dma,
        ],
        compiler_params=pltpu.CompilerParams(
            collective_id=0, has_side_effects=True, vmem_limit_bytes=24 * 1024 * 1024
        ),
    )(*(pltpu.with_memory_space_constraint(a, pltpu.HBM) for a in args))
    return out.reshape(pair_map.shape)


def solution(mesh):
    placed = (P("row", "col", None), P("row", "col"), P(), P(), P(), P(), P(), P(), P())
    return jax.shard_map(local, mesh=mesh, in_specs=placed, out_specs=P("row", "col", None), check_vma=False)
```

```python
import jax
import jax.numpy as jnp
from jax import lax
from jax.experimental import pallas as pl
from jax.experimental.pallas import tpu as pltpu
from jax.sharding import PartitionSpec as P

MESH = pl.DeviceIdType.MESH
PLANES = 8
QUAD = 4
PEERS = 32
HELD = 4
PITCH = 136
NN = (((1,), (0,)), ((), ()))
NT = (((1,), (1,)), ((), ()))
TN = (((0,), (0,)), ((), ()))


def steps(reach):
    every = [(dx, dy, dh) for dx in range(4) for dy in range(4) for dh in range(2) if dx or dy or dh]
    return sorted(every, key=lambda s: reach(min(s[0], 4 - s[0]) + min(s[1], 4 - s[1])))


def dot(a, b, dims):
    return lax.dot_general(a, b, dims, preferred_element_type=jnp.float32)


def halves(a, b):
    low = lax.broadcasted_iota(jnp.int32, a.shape, 1) < 64
    return jnp.where(low, a, pltpu.roll(b, 64, 1)), jnp.where(low, pltpu.roll(a, 64, 1), b)


def kernel(
    x_hbm, mask_hbm, in_gain_hbm, in_bias_hbm, w_proj_hbm, w_gate_hbm, out_gain_hbm, out_bias_hbm, w_out_hbm, out_ref,
    x_ref, mask_ref, in_gain, in_bias, w_proj, w_gate, out_gain, out_bias, w_out, x_sem, in_sem,
    stage, normed, gate, send_r, send_l, recv_r, recv_l, left, right, s_send, s_recv, column,
    send_r_sem, recv_r_sem, send_l_sem, recv_l_sem, up_s, up_r, down_s, down_r, s_s, s_r,
):
    row, col = lax.axis_index("row"), lax.axis_index("col")
    z, quarter = lax.div(row, QUAD), lax.rem(row, QUAD)
    me = col * QUAD + quarter
    x = lax.div(col, 4) * 2 + lax.div(quarter, 2)
    y, core = lax.rem(col, 4), lax.rem(quarter, 2)
    strip = lax.div(col, 2)
    above = {"row": lax.rem(row + QUAD, PLANES * QUAD), "col": col}
    below = {"row": lax.rem(row + (PLANES - 1) * QUAD, PLANES * QUAD), "col": col}

    def peer(other):
        return {"row": z * QUAD + lax.rem(other, QUAD), "col": lax.div(other, QUAD)}

    def each(reach, step):
        for dx, dy, dh in steps(reach):
            to_x, to_y, to_core = lax.rem(x + dx, 4), lax.rem(y + dy, 4), lax.rem(core + dh, 2)
            step(lax.div(to_x, 2) * 16 + to_y * 4 + lax.rem(to_x, 2) * 2 + to_core)

    x_in = pltpu.make_async_copy(x_hbm, x_ref, x_sem)
    small = [
        pltpu.make_async_copy(src, dst, in_sem.at[n])
        for n, (src, dst) in enumerate((
            (in_gain_hbm, in_gain), (in_bias_hbm, in_bias), (w_proj_hbm, w_proj), (mask_hbm, mask_ref),
            (w_gate_hbm, w_gate), (out_gain_hbm, out_gain), (out_bias_hbm, out_bias), (w_out_hbm, w_out),
        ))
    ]
    for copy in (*small[:4], x_in, *small[4:]):
        copy.start()
    barrier = pltpu.get_barrier_semaphore()
    each(lambda hops: -hops, lambda o: pl.semaphore_signal(barrier, inc=1, device_id=peer(o), device_id_type=MESH))
    for neighbour in (above, below):
        pl.semaphore_signal(barrier, inc=1, device_id=neighbour, device_id_type=MESH)

    for copy in small[:4]:
        copy.wait()

    lane_low = lax.broadcasted_iota(jnp.int32, (8, 128), 1) < 64
    mask = mask_ref[...].astype(jnp.float32)
    masked = jnp.concatenate([mask[:8], mask[8:]], axis=1)
    weights = jnp.transpose(w_proj[...].astype(jnp.float32)).astype(jnp.bfloat16)

    def layer_norm_in(t):
        v = jnp.concatenate([x_ref[0, t], x_ref[1, t]], axis=0)
        average = jnp.mean(v, axis=1, keepdims=True)
        variance = jnp.mean(jnp.square(v - average), axis=1, keepdims=True)
        return ((v - average) * lax.rsqrt(variance + 1e-05) * in_gain[...] + in_bias[...]).astype(jnp.bfloat16)

    def project(t, first):
        p = dot(weights[first : first + 256], normed[t], NT)
        side = masked[t : t + 1] * jax.nn.sigmoid(p[:128]) * p[128:]
        stage[pl.ds(t * PITCH, 128), :] = side

    def pack(send):
        for g in range(64):
            pair = [stage[pl.ds(2 * g + e, 8, stride=PITCH), :] for e in range(2)]
            send[g // 2, g % 2] = jnp.concatenate(pair, axis=0).astype(jnp.bfloat16)

    def move(src, dst, send_sem, recv_sem, to):
        return pltpu.make_async_remote_copy(
            src_ref=src, dst_ref=dst, send_sem=send_sem, recv_sem=recv_sem, device_id=to, device_id_type=MESH
        )

    def regroup(recv, strip, store):
        for g in range(2):
            for rr in range(QUAD):
                a = recv[8 * strip + rr, g].astype(jnp.float32)
                b = recv[8 * strip + 4 + rr, g].astype(jnp.float32)
                first, second = halves(a, b)
                for e in range(2):
                    rows = slice(8 * e, 8 * e + 8)
                    tile = jnp.concatenate([first[rows], second[rows]], axis=0).astype(jnp.bfloat16)
                    store(2 * g + e, slice(16 * rr, 16 * rr + 16), tile)

    x_in.wait()
    for t in range(8):
        normed[t] = layer_norm_in(t)
        project(t, 256)
    pack(send_r)
    pl.semaphore_wait(barrier, PEERS - 1 + 2)
    each(
        lambda hops: (1, 2, 3, 4, 0)[hops],
        lambda o: move(send_r.at[o], recv_r.at[me], send_r_sem, recv_r_sem.at[strip], peer(o)).start(),
    )
    recv_r[me] = send_r[me]

    for t in range(8):
        project(t, 0)
    pack(send_l)
    recv_l[me] = send_l[me]

    for copy in small[4:]:
        copy.wait()
    for t in range(8):
        p = jax.nn.sigmoid(dot(normed[t], w_gate[...], NN))
        gate[t] = p[:64]
        gate[t + 8] = p[64:]
    column[0] = jnp.transpose(jnp.broadcast_to(out_gain[...], (128, 128)))
    column[1] = jnp.transpose(jnp.broadcast_to(out_bias[...], (128, 128)))

    def near(e):
        return lax.rem(lax.div(strip, 2) + e // 2, 2) * 2 + lax.rem(strip + e % 2, 2)

    class Stream:
        def __init__(self, sign, to, far, sends, recvs):
            self.sign, self.to, self.far, self.sends, self.recvs = sign, to, far, sends, recvs
            self.rest = (2, 3) if far == 0 else (0, 1)

        def block(self, d):
            return lax.rem(z + (PLANES - d if self.sign > 0 else d), PLANES)

        def copy(self, part, slot):
            return move(part, part, self.sends, self.recvs.at[slot], self.to)

        def strip(self, d, e):
            part = right.at[self.block(d - 1) * 4 + near(e)]
            return self.copy(part if d == 1 else part.at[pl.ds(self.far, 2)], 4 * (d - 1) + e)

        def half(self, n, h):
            return self.copy(right.at[pl.ds(self.block(1) * 4 + 2 * h, 2), self.rest[n]], 20 + 2 * n + h)

    streams = (Stream(1, above, 0, up_s, up_r), Stream(-1, below, 2, down_s, down_r))

    for e in range(4):
        got = near(e)
        arrived = recv_r.at[pl.ds(8 * got, 8 if e else 7)]
        move(arrived, arrived, send_r_sem, recv_r_sem.at[got], above).wait_recv()

        def store_right(ch, rows, tile, got=got):
            right[z * 4 + got, ch, rows] = tile

        regroup(recv_r, got, store_right)
        for stream in streams:
            stream.strip(1, e).start()
        if e == 0:
            each(
                lambda hops: -hops,
                lambda o: move(send_l.at[o], recv_l.at[me], send_l_sem, recv_l_sem, peer(o)).start(),
            )

    def store_left(strip):
        def store(ch, rows, tile):
            left[ch, rows, slice(128 * strip, 128 * strip + 128)] = tile

        return store

    def s_block(block, channels=range(HELD)):
        tiles = []
        for ch in channels:
            r = jnp.concatenate([right[block * 4 + k, ch] for k in range(4)], axis=1)
            s = dot(left[ch], jnp.concatenate([r, r], axis=0), NT)
            tiles.append([
                jnp.where(lane_low, s[16 * rr : 16 * rr + 8], s[16 * rr + 8 : 16 * rr + 16]) for rr in range(QUAD)
            ])
        first, count = channels[0] * 8, len(channels) * 8
        dst = s_recv.at[pl.ds(pl.multiple_of(me * 32 + first, 8), count)]
        for rr in range(QUAD):
            tile = jnp.concatenate([t[rr] for t in tiles], axis=0)
            mine = jnp.logical_and(block == col, quarter == rr)

            @pl.when(mine)
            def _():
                dst[...] = tile

            @pl.when(jnp.logical_not(mine))
            def _():
                src = s_send.at[pl.ds(pl.multiple_of((block * QUAD + rr) * 32 + first, 8), count)]
                src[...] = tile
                move(src, dst, s_s, s_r, {"row": z * QUAD + rr, "col": block}).start()

    def forward(d):
        for e in range(4):
            for stream in streams:
                stream.strip(d, e).wait_recv()
                if d < 5:
                    stream.strip(d + 1, e).start()

    def late(n, h):
        for stream in streams:
            stream.half(n, h).start()

    def s_late(n):
        for stream in streams:
            stream.half(n, 0).wait_recv()
            stream.half(n, 1).wait_recv()
            s_block(stream.block(2), (stream.rest[n],))

    def s_far(d):
        for stream in streams:
            s_block(stream.block(d), range(stream.far, stream.far + 2))

    forward(1)
    late(0, 0)
    arrived = recv_l.at[pl.ds(0, PEERS - 1)]
    move(arrived, arrived, send_l_sem, recv_l_sem, above).wait_recv()
    for k in range(4):
        regroup(recv_l, k, store_left(k))
    s_block(z)
    forward(2)
    late(0, 1)
    for stream in streams:
        s_block(stream.block(1))
    forward(3)
    late(1, 0)
    s_far(2)
    s_far(3)
    forward(4)
    late(1, 1)
    s_late(0)
    s_far(4)
    forward(5)
    s_far(5)
    s_late(1)

    sent = send_r.at[pl.ds(0, PEERS - 1)]
    move(sent, sent, send_r_sem, recv_r_sem.at[0], above).wait_send()
    move(sent, sent, send_l_sem, recv_l_sem, above).wait_send()
    sent = right.at[pl.ds(0, 14)]
    move(sent, sent, up_s, up_r.at[0], above).wait_send()
    move(sent, sent, down_s, down_r.at[0], below).wait_send()
    sent = s_send.at[pl.ds(0, (PEERS - 1) * 32)]
    move(sent, sent, s_s, s_r, above).wait_send()
    arrived = s_recv.at[pl.ds(0, (PEERS - 1) * 32)]
    move(arrived, arrived, s_s, s_r, above).wait_recv()
    for t in range(8):
        v = s_recv[pl.ds(t, 128, stride=8), :]
        average = jnp.mean(v, axis=0, keepdims=True)
        variance = jnp.mean(jnp.square(v - average), axis=0, keepdims=True)
        n = ((v - average) * lax.rsqrt(variance + 1e-05) * column[0] + column[1]).astype(jnp.bfloat16)
        o = dot(n, w_out[...], TN)
        out_ref[0, t] = gate[t] * o[:64]
        out_ref[1, t] = gate[t + 8] * o[64:]


def local(pair_map, pair_mask, in_gain, in_bias, w_proj, w_gate, out_gain, out_bias, w_out):
    f32, bf16 = jnp.float32, jnp.bfloat16
    vmem, dma = pltpu.VMEM, pltpu.SemaphoreType.DMA
    split = (2, 8, 64, 128)
    args = (
        pair_map.reshape(split), pair_mask, in_gain.reshape(1, -1), in_bias.reshape(1, -1), w_proj, w_gate,
        out_gain.reshape(1, -1), out_bias.reshape(1, -1), w_out,
    )
    out = pl.pallas_call(
        kernel,
        out_shape=jax.ShapeDtypeStruct(split, f32),
        in_specs=[pl.BlockSpec(memory_space=pltpu.HBM)] * 9,
        out_specs=pl.BlockSpec(memory_space=vmem),
        scratch_shapes=[
            *(vmem(a.shape, a.dtype) for a in args),
            dma, dma((8,)),
            vmem((8 * PITCH, 128), f32),
            vmem((8, 128, 128), bf16),
            vmem((16, 64, 128), f32),
            vmem((PEERS, 2, 16, 128), bf16),
            vmem((PEERS, 2, 16, 128), bf16),
            vmem((PEERS, 2, 16, 128), bf16),
            vmem((PEERS, 2, 16, 128), bf16),
            vmem((HELD, 64, 512), bf16),
            vmem((PLANES * 4, HELD, 64, 128), bf16),
            vmem((1024, 128), f32),
            vmem((1024, 128), f32),
            vmem((2, 128, 128), f32),
            dma, dma((4,)), dma, dma, dma, dma((24,)), dma, dma((24,)), dma, dma,
        ],
        compiler_params=pltpu.CompilerParams(
            collective_id=0, has_side_effects=True, vmem_limit_bytes=24 * 1024 * 1024
        ),
    )(*(pltpu.with_memory_space_constraint(a, pltpu.HBM) for a in args))
    return out.reshape(pair_map.shape)


def solution(mesh):
    placed = (P("row", "col", None), P("row", "col"), P(), P(), P(), P(), P(), P(), P())
    return jax.shard_map(local, mesh=mesh, in_specs=placed, out_specs=P("row", "col", None), check_vma=False)
```

```python
import jax
import jax.numpy as jnp
from jax import lax
from jax.experimental import pallas as pl
from jax.experimental.pallas import tpu as pltpu
from jax.sharding import PartitionSpec as P

MESH = pl.DeviceIdType.MESH
PLANES = 8
QUAD = 4
PEERS = 32
HELD = 4
PITCH = 136
NN = (((1,), (0,)), ((), ()))
NT = (((1,), (1,)), ((), ()))
TN = (((0,), (0,)), ((), ()))


def steps(reach):
    every = [(dx, dy, dh) for dx in range(4) for dy in range(4) for dh in range(2) if dx or dy or dh]
    return sorted(every, key=lambda s: reach(min(s[0], 4 - s[0]) + min(s[1], 4 - s[1])))


def dot(a, b, dims):
    return lax.dot_general(a, b, dims, preferred_element_type=jnp.float32)


def halves(a, b):
    low = lax.broadcasted_iota(jnp.int32, a.shape, 1) < 64
    return jnp.where(low, a, pltpu.roll(b, 64, 1)), jnp.where(low, pltpu.roll(a, 64, 1), b)


def kernel(
    x_hbm, mask_hbm, in_gain_hbm, in_bias_hbm, w_proj_hbm, w_gate_hbm, out_gain_hbm, out_bias_hbm, w_out_hbm, out_ref,
    x_ref, mask_ref, in_gain, in_bias, w_proj, w_gate, out_gain, out_bias, w_out, x_sem, in_sem,
    stage, normed, gate, send_r, send_l, recv_r, recv_l, raw, recv_x, left, right, s_send, s_recv, column,
    send_r_sem, recv_r_sem, send_l_sem, recv_l_sem, send_x_sem, recv_x_sem, up_s, up_r, down_s, down_r, s_s, s_r,
):
    row, col = lax.axis_index("row"), lax.axis_index("col")
    z, quarter = lax.div(row, QUAD), lax.rem(row, QUAD)
    me = col * QUAD + quarter
    x = lax.div(col, 4) * 2 + lax.div(quarter, 2)
    y, core = lax.rem(col, 4), lax.rem(quarter, 2)
    strip = lax.div(col, 2)
    above = {"row": lax.rem(row + QUAD, PLANES * QUAD), "col": col}
    below = {"row": lax.rem(row + (PLANES - 1) * QUAD, PLANES * QUAD), "col": col}

    def peer(other):
        return {"row": z * QUAD + lax.rem(other, QUAD), "col": lax.div(other, QUAD)}

    def each(reach, step):
        for dx, dy, dh in steps(reach):
            to_x, to_y, to_core = lax.rem(x + dx, 4), lax.rem(y + dy, 4), lax.rem(core + dh, 2)
            step(lax.div(to_x, 2) * 16 + to_y * 4 + lax.rem(to_x, 2) * 2 + to_core)

    x_in = pltpu.make_async_copy(x_hbm, x_ref, x_sem)
    small = [
        pltpu.make_async_copy(src, dst, in_sem.at[n])
        for n, (src, dst) in enumerate((
            (in_gain_hbm, in_gain), (in_bias_hbm, in_bias), (w_proj_hbm, w_proj), (mask_hbm, mask_ref),
            (w_gate_hbm, w_gate), (out_gain_hbm, out_gain), (out_bias_hbm, out_bias), (w_out_hbm, w_out),
        ))
    ]
    for copy in (*small[:4], x_in, *small[4:]):
        copy.start()
    barrier = pltpu.get_barrier_semaphore()
    each(lambda hops: -hops, lambda o: pl.semaphore_signal(barrier, inc=1, device_id=peer(o), device_id_type=MESH))
    for neighbour in (above, below):
        pl.semaphore_signal(barrier, inc=1, device_id=neighbour, device_id_type=MESH)

    for copy in small[:4]:
        copy.wait()

    lane_low = lax.broadcasted_iota(jnp.int32, (8, 128), 1) < 64
    mask = mask_ref[...].astype(jnp.float32)
    masked = jnp.concatenate([mask[:8], mask[8:]], axis=1)
    weights = jnp.transpose(w_proj[...].astype(jnp.float32)).astype(jnp.bfloat16)

    def layer_norm_in(t):
        v = jnp.concatenate([x_ref[0, t], x_ref[1, t]], axis=0)
        average = jnp.mean(v, axis=1, keepdims=True)
        variance = jnp.mean(jnp.square(v - average), axis=1, keepdims=True)
        return ((v - average) * lax.rsqrt(variance + 1e-05) * in_gain[...] + in_bias[...]).astype(jnp.bfloat16)

    def project(t, first):
        p = dot(weights[first : first + 256], normed[t], NT)
        side = masked[t : t + 1] * jax.nn.sigmoid(p[:128]) * p[128:]
        stage[pl.ds(t * PITCH, 128), :] = side

    def pack(send):
        for g in range(64):
            pair = [stage[pl.ds(2 * g + e, 8, stride=PITCH), :] for e in range(2)]
            send[g // 2, g % 2] = jnp.concatenate(pair, axis=0).astype(jnp.bfloat16)

    def move(src, dst, send_sem, recv_sem, to):
        return pltpu.make_async_remote_copy(
            src_ref=src, dst_ref=dst, send_sem=send_sem, recv_sem=recv_sem, device_id=to, device_id_type=MESH
        )

    def regroup(recv, strip, store):
        for g in range(2):
            for rr in range(QUAD):
                a = recv[8 * strip + rr, g].astype(jnp.float32)
                b = recv[8 * strip + 4 + rr, g].astype(jnp.float32)
                first, second = halves(a, b)
                for e in range(2):
                    rows = slice(8 * e, 8 * e + 8)
                    tile = jnp.concatenate([first[rows], second[rows]], axis=0).astype(jnp.bfloat16)
                    store(2 * g + e, slice(16 * rr, 16 * rr + 16), tile)

    def near(e):
        return lax.rem(lax.div(strip, 2) + e // 2, 2) * 2 + lax.rem(strip + e % 2, 2)

    class Stream:
        def __init__(self, sign, to, far, sends, recvs):
            self.sign, self.to, self.far, self.sends, self.recvs = sign, to, far, sends, recvs
            self.rest = (2, 3) if far == 0 else (0, 1)

        def block(self, d):
            return lax.rem(z + (PLANES - d if self.sign > 0 else d), PLANES)

        def raw(self, e):
            at = pl.ds(8 * near(e), 8)
            src, dst = send_r.at[at, self.rest[0] // 2], raw.at[at, self.far // 2]
            return move(src, dst, self.sends, self.recvs.at[24 + e], self.to)

        def strip(self, d, e):
            part = right.at[self.block(d - 1) * 4 + near(e), pl.ds(self.far, 2)]
            return move(part, part, self.sends, self.recvs.at[4 * (d - 1) + e], self.to)

        def half(self, n, h):
            part = right.at[pl.ds(self.block(1) * 4 + 2 * h, 2), self.rest[n]]
            return move(part, part, self.sends, self.recvs.at[20 + 2 * n + h], self.to)

    streams = (Stream(1, above, 0, up_s, up_r), Stream(-1, below, 2, down_s, down_r))

    def pass_on(e):
        for stream in streams:
            stream.raw(e).wait_recv()
        for n in range(0 if e else 1, 8):
            o = 8 * near(e) + lax.rem(me + n, 8)
            move(raw.at[o], recv_x.at[me], send_x_sem, recv_x_sem, peer(o)).start()

    x_in.wait()
    for t in range(8):
        normed[t] = layer_norm_in(t)
        project(t, 256)
    pack(send_r)
    pl.semaphore_wait(barrier, PEERS - 1 + 2)
    for e in (3, 2, 1, 0):
        for stream in streams:
            stream.raw(e).start()
    each(
        lambda hops: (1, 2, 3, 4, 0)[hops],
        lambda o: move(send_r.at[o], recv_r.at[me], send_r_sem, recv_r_sem.at[strip], peer(o)).start(),
    )
    recv_r[me] = send_r[me]

    for t in range(8):
        project(t, 0)
    pack(send_l)
    recv_l[me] = send_l[me]

    for copy in small[4:]:
        copy.wait()
    for t in range(8):
        p = jax.nn.sigmoid(dot(normed[t], w_gate[...], NN))
        gate[t] = p[:64]
        gate[t + 8] = p[64:]
    column[0] = jnp.transpose(jnp.broadcast_to(out_gain[...], (128, 128)))
    column[1] = jnp.transpose(jnp.broadcast_to(out_bias[...], (128, 128)))

    for e in range(4):
        got = near(e)
        arrived = recv_r.at[pl.ds(8 * got, 8 if e else 7)]
        move(arrived, arrived, send_r_sem, recv_r_sem.at[got], above).wait_recv()

        def store_right(ch, rows, tile, got=got):
            right[z * 4 + got, ch, rows] = tile

        regroup(recv_r, got, store_right)
        for stream in streams:
            stream.strip(1, e).start()
        if e == 0:
            pass_on(3)
            pass_on(2)
        if e == 2:
            pass_on(1)
            pass_on(0)
            recv_x[me] = raw[me]
            each(
                lambda hops: -hops,
                lambda o: move(send_l.at[o], recv_l.at[me], send_l_sem, recv_l_sem, peer(o)).start(),
            )

    def store_left(strip):
        def store(ch, rows, tile):
            left[ch, rows, slice(128 * strip, 128 * strip + 128)] = tile

        return store

    def s_block(block, channels=range(HELD)):
        tiles = []
        for ch in channels:
            r = jnp.concatenate([right[block * 4 + k, ch] for k in range(4)], axis=1)
            s = dot(left[ch], jnp.concatenate([r, r], axis=0), NT)
            tiles.append([
                jnp.where(lane_low, s[16 * rr : 16 * rr + 8], s[16 * rr + 8 : 16 * rr + 16]) for rr in range(QUAD)
            ])
        first, count = channels[0] * 8, len(channels) * 8
        dst = s_recv.at[pl.ds(pl.multiple_of(me * 32 + first, 8), count)]
        for rr in range(QUAD):
            tile = jnp.concatenate([t[rr] for t in tiles], axis=0)
            mine = jnp.logical_and(block == col, quarter == rr)

            @pl.when(mine)
            def _():
                dst[...] = tile

            @pl.when(jnp.logical_not(mine))
            def _():
                src = s_send.at[pl.ds(pl.multiple_of((block * QUAD + rr) * 32 + first, 8), count)]
                src[...] = tile
                move(src, dst, s_s, s_r, {"row": z * QUAD + rr, "col": block}).start()

    def forward(d):
        for e in range(4):
            for stream in streams:
                stream.strip(d, e).wait_recv()
                if d < 5:
                    stream.strip(d + 1, e).start()

    def late(n, h):
        for stream in streams:
            stream.half(n, h).start()

    def s_late(n):
        for stream in streams:
            stream.half(n, 0).wait_recv()
            stream.half(n, 1).wait_recv()
            s_block(stream.block(2), (stream.rest[n],))

    def s_far(d):
        for stream in streams:
            s_block(stream.block(d), range(stream.far, stream.far + 2))

    forward(1)
    forward(2)
    arrived = recv_x.at[pl.ds(0, PEERS - 1)]
    move(arrived, arrived, send_x_sem, recv_x_sem, above).wait_recv()
    for k in range(4):

        def store_next(ch, rows, tile, k=k):
            stream = streams[ch // 2]
            right[stream.block(1) * 4 + k, stream.rest[ch % 2], rows] = tile

        regroup(recv_x, k, store_next)
    late(0, 0)
    late(0, 1)
    arrived = recv_l.at[pl.ds(0, PEERS - 1)]
    move(arrived, arrived, send_l_sem, recv_l_sem, above).wait_recv()
    for k in range(4):
        regroup(recv_l, k, store_left(k))
    s_block(z)
    forward(3)
    late(1, 0)
    for stream in streams:
        s_block(stream.block(1))
    s_far(2)
    forward(4)
    late(1, 1)
    s_far(3)
    s_late(0)
    s_far(4)
    forward(5)
    s_far(5)
    s_late(1)

    sent = send_r.at[pl.ds(0, PEERS - 1)]
    move(sent, sent, send_r_sem, recv_r_sem.at[0], above).wait_send()
    move(sent, sent, send_l_sem, recv_l_sem, above).wait_send()
    move(sent, sent, send_x_sem, recv_x_sem, above).wait_send()
    sent = right.at[pl.ds(0, 14)]
    move(sent, sent, up_s, up_r.at[0], above).wait_send()
    move(sent, sent, down_s, down_r.at[0], below).wait_send()
    sent = s_send.at[pl.ds(0, (PEERS - 1) * 32)]
    move(sent, sent, s_s, s_r, above).wait_send()
    arrived = s_recv.at[pl.ds(0, (PEERS - 1) * 32)]
    move(arrived, arrived, s_s, s_r, above).wait_recv()
    for t in range(8):
        v = s_recv[pl.ds(t, 128, stride=8), :]
        average = jnp.mean(v, axis=0, keepdims=True)
        variance = jnp.mean(jnp.square(v - average), axis=0, keepdims=True)
        n = ((v - average) * lax.rsqrt(variance + 1e-05) * column[0] + column[1]).astype(jnp.bfloat16)
        o = dot(n, w_out[...], TN)
        out_ref[0, t] = gate[t] * o[:64]
        out_ref[1, t] = gate[t + 8] * o[64:]


def local(pair_map, pair_mask, in_gain, in_bias, w_proj, w_gate, out_gain, out_bias, w_out):
    f32, bf16 = jnp.float32, jnp.bfloat16
    vmem, dma = pltpu.VMEM, pltpu.SemaphoreType.DMA
    split = (2, 8, 64, 128)
    args = (
        pair_map.reshape(split), pair_mask, in_gain.reshape(1, -1), in_bias.reshape(1, -1), w_proj, w_gate,
        out_gain.reshape(1, -1), out_bias.reshape(1, -1), w_out,
    )
    out = pl.pallas_call(
        kernel,
        out_shape=jax.ShapeDtypeStruct(split, f32),
        in_specs=[pl.BlockSpec(memory_space=pltpu.HBM)] * 9,
        out_specs=pl.BlockSpec(memory_space=vmem),
        scratch_shapes=[
            *(vmem(a.shape, a.dtype) for a in args),
            dma, dma((8,)),
            vmem((8 * PITCH, 128), f32),
            vmem((8, 128, 128), bf16),
            vmem((16, 64, 128), f32),
            vmem((PEERS, 2, 16, 128), bf16),
            vmem((PEERS, 2, 16, 128), bf16),
            vmem((PEERS, 2, 16, 128), bf16),
            vmem((PEERS, 2, 16, 128), bf16),
            vmem((PEERS, 2, 16, 128), bf16),
            vmem((PEERS, 2, 16, 128), bf16),
            vmem((HELD, 64, 512), bf16),
            vmem((PLANES * 4, HELD, 64, 128), bf16),
            vmem((1024, 128), f32),
            vmem((1024, 128), f32),
            vmem((2, 128, 128), f32),
            dma, dma((4,)), dma, dma, dma, dma, dma, dma((28,)), dma, dma((28,)), dma, dma,
        ],
        compiler_params=pltpu.CompilerParams(
            collective_id=0, has_side_effects=True, vmem_limit_bytes=24 * 1024 * 1024
        ),
    )(*(pltpu.with_memory_space_constraint(a, pltpu.HBM) for a in args))
    return out.reshape(pair_map.shape)


def solution(mesh):
    placed = (P("row", "col", None), P("row", "col"), P(), P(), P(), P(), P(), P(), P())
    return jax.shard_map(local, mesh=mesh, in_specs=placed, out_specs=P("row", "col", None), check_vma=False)
```

```python
import jax
import jax.numpy as jnp
from jax import lax
from jax.experimental import pallas as pl
from jax.experimental.pallas import tpu as pltpu
from jax.sharding import PartitionSpec as P

MESH = pl.DeviceIdType.MESH
PLANES = 8
QUAD = 4
PEERS = 32
HELD = 4
PITCH = 136
NN = (((1,), (0,)), ((), ()))
NT = (((1,), (1,)), ((), ()))
TN = (((0,), (0,)), ((), ()))


def steps(reach):
    every = [(dx, dy, dh) for dx in range(4) for dy in range(4) for dh in range(2) if dx or dy or dh]
    return sorted(every, key=lambda s: reach(min(s[0], 4 - s[0]) + min(s[1], 4 - s[1])))


def dot(a, b, dims):
    return lax.dot_general(a, b, dims, preferred_element_type=jnp.float32)


def halves(a, b):
    low = lax.broadcasted_iota(jnp.int32, a.shape, 1) < 64
    return jnp.where(low, a, pltpu.roll(b, 64, 1)), jnp.where(low, pltpu.roll(a, 64, 1), b)


def kernel(
    x_hbm, mask_hbm, in_gain_hbm, in_bias_hbm, w_proj_hbm, w_gate_hbm, out_gain_hbm, out_bias_hbm, w_out_hbm, out_ref,
    x_ref, mask_ref, in_gain, in_bias, w_proj, w_gate, out_gain, out_bias, w_out, x_sem, in_sem,
    stage, normed, gate, send_r, send_l, recv_r, recv_l, raw, recv_x, left, right, s_send, s_recv, column,
    send_r_sem, recv_r_sem, send_l_sem, recv_l_sem, send_x_sem, recv_x_sem, up_s, up_r, down_s, down_r, s_s, s_r,
):
    row, col = lax.axis_index("row"), lax.axis_index("col")
    z, quarter = lax.div(row, QUAD), lax.rem(row, QUAD)
    me = col * QUAD + quarter
    x = lax.div(col, 4) * 2 + lax.div(quarter, 2)
    y, core = lax.rem(col, 4), lax.rem(quarter, 2)
    strip = lax.div(col, 2)
    above = {"row": lax.rem(row + QUAD, PLANES * QUAD), "col": col}
    below = {"row": lax.rem(row + (PLANES - 1) * QUAD, PLANES * QUAD), "col": col}

    def peer(other):
        return {"row": z * QUAD + lax.rem(other, QUAD), "col": lax.div(other, QUAD)}

    def each(reach, step):
        for dx, dy, dh in steps(reach):
            to_x, to_y, to_core = lax.rem(x + dx, 4), lax.rem(y + dy, 4), lax.rem(core + dh, 2)
            step(lax.div(to_x, 2) * 16 + to_y * 4 + lax.rem(to_x, 2) * 2 + to_core)

    x_in = pltpu.make_async_copy(x_hbm, x_ref, x_sem)
    small = [
        pltpu.make_async_copy(src, dst, in_sem.at[n])
        for n, (src, dst) in enumerate((
            (in_gain_hbm, in_gain), (in_bias_hbm, in_bias), (w_proj_hbm, w_proj), (mask_hbm, mask_ref),
            (w_gate_hbm, w_gate), (out_gain_hbm, out_gain), (out_bias_hbm, out_bias), (w_out_hbm, w_out),
        ))
    ]
    for copy in (*small[:4], x_in, *small[4:]):
        copy.start()
    barrier = pltpu.get_barrier_semaphore()
    each(lambda hops: -hops, lambda o: pl.semaphore_signal(barrier, inc=1, device_id=peer(o), device_id_type=MESH))
    for neighbour in (above, below):
        pl.semaphore_signal(barrier, inc=1, device_id=neighbour, device_id_type=MESH)

    for copy in small[:4]:
        copy.wait()

    lane_low = lax.broadcasted_iota(jnp.int32, (8, 128), 1) < 64
    mask = mask_ref[...].astype(jnp.float32)
    masked = jnp.concatenate([mask[:8], mask[8:]], axis=1)
    weights = jnp.transpose(w_proj[...].astype(jnp.float32)).astype(jnp.bfloat16)

    def layer_norm_in(t):
        v = jnp.concatenate([x_ref[0, t], x_ref[1, t]], axis=0)
        average = jnp.mean(v, axis=1, keepdims=True)
        variance = jnp.mean(jnp.square(v - average), axis=1, keepdims=True)
        return ((v - average) * lax.rsqrt(variance + 1e-05) * in_gain[...] + in_bias[...]).astype(jnp.bfloat16)

    def project(t, first):
        p = dot(weights[first : first + 256], normed[t], NT)
        side = masked[t : t + 1] * jax.nn.sigmoid(p[:128]) * p[128:]
        stage[pl.ds(t * PITCH, 128), :] = side

    def pack(send):
        for g in range(64):
            pair = [stage[pl.ds(2 * g + e, 8, stride=PITCH), :] for e in range(2)]
            send[g // 2, g % 2] = jnp.concatenate(pair, axis=0).astype(jnp.bfloat16)

    def move(src, dst, send_sem, recv_sem, to):
        return pltpu.make_async_remote_copy(
            src_ref=src, dst_ref=dst, send_sem=send_sem, recv_sem=recv_sem, device_id=to, device_id_type=MESH
        )

    def regroup(recv, strip, store):
        for g in range(2):
            for rr in range(QUAD):
                a = recv[8 * strip + rr, g].astype(jnp.float32)
                b = recv[8 * strip + 4 + rr, g].astype(jnp.float32)
                first, second = halves(a, b)
                for e in range(2):
                    rows = slice(8 * e, 8 * e + 8)
                    tile = jnp.concatenate([first[rows], second[rows]], axis=0).astype(jnp.bfloat16)
                    store(2 * g + e, slice(16 * rr, 16 * rr + 16), tile)

    def near(e):
        return lax.rem(lax.div(strip, 2) + e // 2, 2) * 2 + lax.rem(strip + e % 2, 2)

    class Stream:
        def __init__(self, sign, to, far, sends, recvs):
            self.sign, self.to, self.far, self.sends, self.recvs = sign, to, far, sends, recvs
            self.rest = (2, 3) if far == 0 else (0, 1)

        def block(self, d):
            return lax.rem(z + (PLANES - d if self.sign > 0 else d), PLANES)

        def raw(self, e):
            at = pl.ds(8 * near(e), 8)
            src, dst = send_r.at[at, self.rest[0] // 2], raw.at[at, self.far // 2]
            return move(src, dst, self.sends, self.recvs.at[24 + e], self.to)

        def strip(self, d, e):
            part = right.at[self.block(d - 1) * 4 + near(e), pl.ds(self.far, 2)]
            return move(part, part, self.sends, self.recvs.at[4 * (d - 1) + e], self.to)

        def half(self, n, h):
            part = right.at[pl.ds(self.block(1) * 4 + 2 * h, 2), self.rest[n]]
            return move(part, part, self.sends, self.recvs.at[20 + 2 * n + h], self.to)

    streams = (Stream(1, above, 0, up_s, up_r), Stream(-1, below, 2, down_s, down_r))

    def pass_on(e):
        for stream in streams:
            stream.raw(e).wait_recv()
        for n in range(0 if e else 1, 8):
            o = 8 * near(e) + lax.rem(me + n, 8)
            move(raw.at[o], recv_x.at[me], send_x_sem, recv_x_sem, peer(o)).start()

    x_in.wait()
    for t in range(8):
        normed[t] = layer_norm_in(t)
        project(t, 256)
    pack(send_r)
    pl.semaphore_wait(barrier, PEERS - 1 + 2)
    for e in (3, 2, 1, 0):
        for stream in streams:
            stream.raw(e).start()
    each(
        lambda hops: (1, 2, 3, 4, 0)[hops],
        lambda o: move(send_r.at[o], recv_r.at[me], send_r_sem, recv_r_sem.at[strip], peer(o)).start(),
    )
    recv_r[me] = send_r[me]

    for t in range(8):
        project(t, 0)
    pack(send_l)
    recv_l[me] = send_l[me]

    for copy in small[4:]:
        copy.wait()
    for t in range(8):
        p = jax.nn.sigmoid(dot(normed[t], w_gate[...], NN))
        gate[t] = p[:64]
        gate[t + 8] = p[64:]
    column[0] = jnp.transpose(jnp.broadcast_to(out_gain[...], (128, 128)))
    column[1] = jnp.transpose(jnp.broadcast_to(out_bias[...], (128, 128)))

    for e in range(4):
        got = near(e)
        arrived = recv_r.at[pl.ds(8 * got, 8 if e else 7)]
        move(arrived, arrived, send_r_sem, recv_r_sem.at[got], above).wait_recv()

        def store_right(ch, rows, tile, got=got):
            right[z * 4 + got, ch, rows] = tile

        regroup(recv_r, got, store_right)
        for stream in streams:
            stream.strip(1, e).start()
        if e == 0:
            pass_on(3)
            pass_on(2)
        if e == 2:
            pass_on(1)
            pass_on(0)
            recv_x[me] = raw[me]
            each(
                lambda hops: -hops,
                lambda o: move(send_l.at[o], recv_l.at[me], send_l_sem, recv_l_sem, peer(o)).start(),
            )

    def store_left(strip):
        def store(ch, rows, tile):
            left[ch, rows, slice(128 * strip, 128 * strip + 128)] = tile

        return store

    def sums(*parts):
        done = []
        for block, channels in parts:
            tiles = []
            for ch in channels:
                r = jnp.concatenate([right[block * 4 + k, ch] for k in range(4)], axis=1)
                s = dot(left[ch], jnp.concatenate([r, r], axis=0), NT)
                tiles.append([
                    jnp.where(lane_low, s[16 * rr : 16 * rr + 8], s[16 * rr + 8 : 16 * rr + 16]) for rr in range(QUAD)
                ])
            done.append([jnp.concatenate([t[rr] for t in tiles], axis=0) for rr in range(QUAD)])
        for (block, channels), tiles in zip(parts, done):
            first, count = channels[0] * 8, len(channels) * 8
            dst = s_recv.at[pl.ds(pl.multiple_of(me * 32 + first, 8), count)]
            for rr in range(QUAD):
                src = s_send.at[pl.ds(pl.multiple_of((block * QUAD + rr) * 32 + first, 8), count)]
                src[...] = tiles[rr]
            for rr in range(QUAD):
                src = s_send.at[pl.ds(pl.multiple_of((block * QUAD + rr) * 32 + first, 8), count)]
                mine = jnp.logical_and(block == col, quarter == rr)

                @pl.when(mine)
                def _():
                    dst[...] = src[...]

                @pl.when(jnp.logical_not(mine))
                def _():
                    move(src, dst, s_s, s_r, {"row": z * QUAD + rr, "col": block}).start()

    def forward(d):
        for e in range(4):
            for stream in streams:
                stream.strip(d, e).wait_recv()
                if d < 5:
                    stream.strip(d + 1, e).start()

    def late(n, h):
        for stream in streams:
            stream.half(n, h).start()

    def s_late(n):
        for stream in streams:
            stream.half(n, 0).wait_recv()
            stream.half(n, 1).wait_recv()
        sums(*((stream.block(2), (stream.rest[n],)) for stream in streams))

    def s_far(d):
        sums(*((stream.block(d), range(stream.far, stream.far + 2)) for stream in streams))

    forward(1)
    forward(2)
    forward(3)
    arrived = recv_x.at[pl.ds(0, PEERS - 1)]
    move(arrived, arrived, send_x_sem, recv_x_sem, above).wait_recv()
    for k in range(4):

        def store_next(ch, rows, tile, k=k):
            stream = streams[ch // 2]
            right[stream.block(1) * 4 + k, stream.rest[ch % 2], rows] = tile

        regroup(recv_x, k, store_next)
    late(0, 0)
    late(0, 1)
    late(1, 0)
    arrived = recv_l.at[pl.ds(0, PEERS - 1)]
    move(arrived, arrived, send_l_sem, recv_l_sem, above).wait_recv()
    for k in range(4):
        regroup(recv_l, k, store_left(k))
    sums((z, range(HELD)))
    sums(*((stream.block(1), range(HELD)) for stream in streams))
    forward(4)
    late(1, 1)
    s_far(2)
    s_far(3)
    s_late(0)
    s_far(4)
    forward(5)
    s_far(5)
    s_late(1)

    sent = send_r.at[pl.ds(0, PEERS - 1)]
    move(sent, sent, send_r_sem, recv_r_sem.at[0], above).wait_send()
    move(sent, sent, send_l_sem, recv_l_sem, above).wait_send()
    move(sent, sent, send_x_sem, recv_x_sem, above).wait_send()
    sent = right.at[pl.ds(0, 14)]
    move(sent, sent, up_s, up_r.at[0], above).wait_send()
    move(sent, sent, down_s, down_r.at[0], below).wait_send()
    sent = s_send.at[pl.ds(0, (PEERS - 1) * 32)]
    move(sent, sent, s_s, s_r, above).wait_send()
    arrived = s_recv.at[pl.ds(0, (PEERS - 1) * 32)]
    move(arrived, arrived, s_s, s_r, above).wait_recv()
    for t in range(8):
        v = s_recv[pl.ds(t, 128, stride=8), :]
        average = jnp.mean(v, axis=0, keepdims=True)
        variance = jnp.mean(jnp.square(v - average), axis=0, keepdims=True)
        n = ((v - average) * lax.rsqrt(variance + 1e-05) * column[0] + column[1]).astype(jnp.bfloat16)
        o = dot(n, w_out[...], TN)
        out_ref[0, t] = gate[t] * o[:64]
        out_ref[1, t] = gate[t + 8] * o[64:]


def local(pair_map, pair_mask, in_gain, in_bias, w_proj, w_gate, out_gain, out_bias, w_out):
    f32, bf16 = jnp.float32, jnp.bfloat16
    vmem, dma = pltpu.VMEM, pltpu.SemaphoreType.DMA
    split = (2, 8, 64, 128)
    args = (
        pair_map.reshape(split), pair_mask, in_gain.reshape(1, -1), in_bias.reshape(1, -1), w_proj, w_gate,
        out_gain.reshape(1, -1), out_bias.reshape(1, -1), w_out,
    )
    out = pl.pallas_call(
        kernel,
        out_shape=jax.ShapeDtypeStruct(split, f32),
        in_specs=[pl.BlockSpec(memory_space=pltpu.HBM)] * 9,
        out_specs=pl.BlockSpec(memory_space=vmem),
        scratch_shapes=[
            *(vmem(a.shape, a.dtype) for a in args),
            dma, dma((8,)),
            vmem((8 * PITCH, 128), f32),
            vmem((8, 128, 128), bf16),
            vmem((16, 64, 128), f32),
            vmem((PEERS, 2, 16, 128), bf16),
            vmem((PEERS, 2, 16, 128), bf16),
            vmem((PEERS, 2, 16, 128), bf16),
            vmem((PEERS, 2, 16, 128), bf16),
            vmem((PEERS, 2, 16, 128), bf16),
            vmem((PEERS, 2, 16, 128), bf16),
            vmem((HELD, 64, 512), bf16),
            vmem((PLANES * 4, HELD, 64, 128), bf16),
            vmem((1024, 128), f32),
            vmem((1024, 128), f32),
            vmem((2, 128, 128), f32),
            dma, dma((4,)), dma, dma, dma, dma, dma, dma((28,)), dma, dma((28,)), dma, dma,
        ],
        compiler_params=pltpu.CompilerParams(
            collective_id=0, has_side_effects=True, vmem_limit_bytes=24 * 1024 * 1024
        ),
    )(*(pltpu.with_memory_space_constraint(a, pltpu.HBM) for a in args))
    return out.reshape(pair_map.shape)


def solution(mesh):
    placed = (P("row", "col", None), P("row", "col"), P(), P(), P(), P(), P(), P(), P())
    return jax.shard_map(local, mesh=mesh, in_specs=placed, out_specs=P("row", "col", None), check_vma=False)
```

```python
import jax
import jax.numpy as jnp
from jax import lax
from jax.experimental import pallas as pl
from jax.experimental.pallas import tpu as pltpu
from jax.sharding import PartitionSpec as P

MESH = pl.DeviceIdType.MESH
PLANES = 8
QUAD = 4
PEERS = 32
HELD = 4
PITCH = 136
NN = (((1,), (0,)), ((), ()))
NT = (((1,), (1,)), ((), ()))
TN = (((0,), (0,)), ((), ()))


def steps(reach):
    every = [(dx, dy, dh) for dx in range(4) for dy in range(4) for dh in range(2) if dx or dy or dh]
    return sorted(every, key=lambda s: reach(min(s[0], 4 - s[0]) + min(s[1], 4 - s[1])))


def dot(a, b, dims):
    return lax.dot_general(a, b, dims, preferred_element_type=jnp.float32)


def halves(a, b):
    low = lax.broadcasted_iota(jnp.int32, a.shape, 1) < 64
    return jnp.where(low, a, pltpu.roll(b, 64, 1)), jnp.where(low, pltpu.roll(a, 64, 1), b)


def kernel(
    x_hbm, mask_hbm, in_gain_hbm, in_bias_hbm, w_proj_hbm, w_gate_hbm, out_gain_hbm, out_bias_hbm, w_out_hbm, out_ref,
    x_ref, mask_ref, in_gain, in_bias, w_proj, w_gate, out_gain, out_bias, w_out, x_sem, in_sem,
    stage, normed, gate, send_r, send_l, recv_r, recv_l, raw, recv_x, left, right, s_send, s_recv, column,
    send_r_sem, recv_r_sem, send_l_sem, recv_l_sem, send_x_sem, recv_x_sem, up_s, up_r, down_s, down_r, s_s, s_r,
):
    row, col = lax.axis_index("row"), lax.axis_index("col")
    z, quarter = lax.div(row, QUAD), lax.rem(row, QUAD)
    me = col * QUAD + quarter
    x = lax.div(col, 4) * 2 + lax.div(quarter, 2)
    y, core = lax.rem(col, 4), lax.rem(quarter, 2)
    strip = lax.div(col, 2)
    above = {"row": lax.rem(row + QUAD, PLANES * QUAD), "col": col}
    below = {"row": lax.rem(row + (PLANES - 1) * QUAD, PLANES * QUAD), "col": col}

    def peer(other):
        return {"row": z * QUAD + lax.rem(other, QUAD), "col": lax.div(other, QUAD)}

    at_x = [lax.rem(x + n, 4) for n in range(4)]
    at_y = [lax.rem(y + n, 4) for n in range(4)]
    at_core = [core, 1 - core]
    pair_x, odd_x = [lax.div(v, 2) * 4 for v in at_x], [lax.rem(v, 2) * 2 for v in at_x]
    row_x = [z * QUAD + v for v in odd_x]
    slot_x = [4 * p + q for p, q in zip(pair_x, odd_x)]
    slot_y = [4 * v for v in at_y]

    def each(reach, step):
        for dx, dy, dh in steps(reach):
            to = {"row": row_x[dx] + at_core[dh], "col": pair_x[dx] + at_y[dy]}
            step(slot_x[dx] + slot_y[dy] + at_core[dh], to)

    x_in = pltpu.make_async_copy(x_hbm, x_ref, x_sem)
    small = [
        pltpu.make_async_copy(src, dst, in_sem.at[n])
        for n, (src, dst) in enumerate((
            (in_gain_hbm, in_gain), (in_bias_hbm, in_bias), (w_proj_hbm, w_proj), (mask_hbm, mask_ref),
            (w_gate_hbm, w_gate), (out_gain_hbm, out_gain), (out_bias_hbm, out_bias), (w_out_hbm, w_out),
        ))
    ]
    for copy in (*small[:4], x_in, *small[4:]):
        copy.start()
    barrier = pltpu.get_barrier_semaphore()
    each(lambda hops: -hops, lambda _, to: pl.semaphore_signal(barrier, inc=1, device_id=to, device_id_type=MESH))
    for neighbour in (above, below):
        pl.semaphore_signal(barrier, inc=1, device_id=neighbour, device_id_type=MESH)

    for copy in small[:4]:
        copy.wait()

    lane_low = lax.broadcasted_iota(jnp.int32, (8, 128), 1) < 64
    mask = mask_ref[...].astype(jnp.float32)
    masked = jnp.concatenate([mask[:8], mask[8:]], axis=1)
    weights = jnp.transpose(w_proj[...].astype(jnp.float32)).astype(jnp.bfloat16)

    def layer_norm_in(t):
        v = jnp.concatenate([x_ref[0, t], x_ref[1, t]], axis=0)
        average = jnp.mean(v, axis=1, keepdims=True)
        variance = jnp.mean(jnp.square(v - average), axis=1, keepdims=True)
        return ((v - average) * lax.rsqrt(variance + 1e-05) * in_gain[...] + in_bias[...]).astype(jnp.bfloat16)

    def project(t, first):
        p = dot(weights[first : first + 256], normed[t], NT)
        side = masked[t : t + 1] * jax.nn.sigmoid(p[:128]) * p[128:]
        stage[pl.ds(t * PITCH, 128), :] = side

    def pack(send):
        for g in range(64):
            pair = [stage[pl.ds(2 * g + e, 8, stride=PITCH), :] for e in range(2)]
            send[g // 2, g % 2] = jnp.concatenate(pair, axis=0).astype(jnp.bfloat16)

    def move(src, dst, send_sem, recv_sem, to):
        return pltpu.make_async_remote_copy(
            src_ref=src, dst_ref=dst, send_sem=send_sem, recv_sem=recv_sem, device_id=to, device_id_type=MESH
        )

    def regroup(recv, strip, store):
        for g in range(2):
            for rr in range(QUAD):
                a = recv[8 * strip + rr, g].astype(jnp.float32)
                b = recv[8 * strip + 4 + rr, g].astype(jnp.float32)
                first, second = halves(a, b)
                for e in range(2):
                    rows = slice(8 * e, 8 * e + 8)
                    tile = jnp.concatenate([first[rows], second[rows]], axis=0).astype(jnp.bfloat16)
                    store(2 * g + e, slice(16 * rr, 16 * rr + 16), tile)

    def near(e):
        return lax.rem(lax.div(strip, 2) + e // 2, 2) * 2 + lax.rem(strip + e % 2, 2)

    class Stream:
        def __init__(self, sign, to, far, sends, recvs):
            self.sign, self.to, self.far, self.sends, self.recvs = sign, to, far, sends, recvs
            self.rest = (2, 3) if far == 0 else (0, 1)

        def block(self, d):
            return lax.rem(z + (PLANES - d if self.sign > 0 else d), PLANES)

        def raw(self, e):
            at = pl.ds(8 * near(e), 8)
            src, dst = send_r.at[at, self.rest[0] // 2], raw.at[at, self.far // 2]
            return move(src, dst, self.sends, self.recvs.at[17], self.to)

        def strip(self, d, e):
            part = right.at[self.block(d - 1) * 4 + near(e), pl.ds(self.far, 2)]
            return move(part, part, self.sends, self.recvs.at[4 * (d - 1) + e if d < 5 else 16], self.to)

        def half(self, n, h):
            part = right.at[pl.ds(self.block(1) * 4 + 2 * h, 2), self.rest[n]]
            return move(part, part, self.sends, self.recvs.at[18 + n], self.to)

        def wait(self, part, slot):
            move(part, part, self.sends, self.recvs.at[slot], self.to).wait_recv()

    streams = (Stream(1, above, 0, up_s, up_r), Stream(-1, below, 2, down_s, down_r))

    def pass_on(e):
        for n in range(0 if e else 1, 8):
            o = 8 * near(e) + lax.rem(me + n, 8)
            move(raw.at[o], recv_x.at[me], send_x_sem, recv_x_sem, peer(o)).start()

    x_in.wait()
    for t in range(8):
        normed[t] = layer_norm_in(t)
        project(t, 256)
    pack(send_r)
    pl.semaphore_wait(barrier, PEERS - 1 + 2)
    for e in (3, 2, 1, 0):
        for stream in streams:
            stream.raw(e).start()
    each(
        lambda hops: (1, 2, 3, 4, 0)[hops],
        lambda o, to: move(send_r.at[o], recv_r.at[me], send_r_sem, recv_r_sem.at[strip], to).start(),
    )
    recv_r[me] = send_r[me]

    for t in range(8):
        project(t, 0)
    pack(send_l)
    recv_l[me] = send_l[me]

    for copy in small[4:]:
        copy.wait()
    for t in range(8):
        p = jax.nn.sigmoid(dot(normed[t], w_gate[...], NN))
        gate[t] = p[:64]
        gate[t + 8] = p[64:]
    column[0] = jnp.transpose(jnp.broadcast_to(out_gain[...], (128, 128)))
    column[1] = jnp.transpose(jnp.broadcast_to(out_bias[...], (128, 128)))

    for e in range(4):
        got = near(e)
        arrived = recv_r.at[pl.ds(8 * got, 8 if e else 7)]
        move(arrived, arrived, send_r_sem, recv_r_sem.at[got], above).wait_recv()

        def store_right(ch, rows, tile, got=got):
            right[z * 4 + got, ch, rows] = tile

        regroup(recv_r, got, store_right)
        for stream in streams:
            stream.strip(1, e).start()
        if e == 1:
            for stream in streams:
                stream.wait(raw.at[pl.ds(0, 16)], 17)
            for part in (3, 2, 1, 0):
                pass_on(part)
            recv_x[me] = raw[me]
        if e == 2:
            each(
                lambda hops: -hops,
                lambda o, to: move(send_l.at[o], recv_l.at[me], send_l_sem, recv_l_sem, to).start(),
            )

    def store_left(strip):
        def store(ch, rows, tile):
            left[ch, rows, slice(128 * strip, 128 * strip + 128)] = tile

        return store

    def sums(*parts):
        done = []
        for block, channels in parts:
            tiles = []
            for ch in channels:
                r = jnp.concatenate([right[block * 4 + k, ch] for k in range(4)], axis=1)
                s = dot(left[ch], jnp.concatenate([r, r], axis=0), NT)
                tiles.append([
                    jnp.where(lane_low, s[16 * rr : 16 * rr + 8], s[16 * rr + 8 : 16 * rr + 16]) for rr in range(QUAD)
                ])
            done.append([jnp.concatenate([t[rr] for t in tiles], axis=0) for rr in range(QUAD)])
        for (block, channels), tiles in zip(parts, done):
            first, count = channels[0] * 8, len(channels) * 8
            dst = s_recv.at[pl.ds(pl.multiple_of(me * 32 + first, 8), count)]
            for rr in range(QUAD):
                src = s_send.at[pl.ds(pl.multiple_of((block * QUAD + rr) * 32 + first, 8), count)]
                src[...] = tiles[rr]
            for rr in range(QUAD):
                src = s_send.at[pl.ds(pl.multiple_of((block * QUAD + rr) * 32 + first, 8), count)]
                mine = jnp.logical_and(block == col, quarter == rr)

                @pl.when(mine)
                def _():
                    dst[...] = src[...]

                @pl.when(jnp.logical_not(mine))
                def _():
                    move(src, dst, s_s, s_r, {"row": z * QUAD + rr, "col": block}).start()

    def forward(d, strips=range(4)):
        for e in strips:
            for stream in streams:
                stream.strip(d, e).wait_recv()
                stream.strip(d + 1, e).start()

    def late(n, h):
        for stream in streams:
            stream.half(n, h).start()

    def s_late(n):
        for stream in streams:
            stream.wait(right.at[0], 18 + n)
        sums(*((stream.block(2), (stream.rest[n],)) for stream in streams))

    def s_far(d):
        sums(*((stream.block(d), range(stream.far, stream.far + 2)) for stream in streams))

    forward(1)
    forward(2)
    forward(3, range(1))
    arrived = recv_x.at[pl.ds(0, PEERS - 1)]
    move(arrived, arrived, send_x_sem, recv_x_sem, above).wait_recv()
    for k in range(4):

        def store_next(ch, rows, tile, k=k):
            stream = streams[ch // 2]
            right[stream.block(1) * 4 + k, stream.rest[ch % 2], rows] = tile

        regroup(recv_x, k, store_next)
    late(0, 0)
    forward(3, range(1, 4))
    late(0, 1)
    late(1, 0)
    arrived = recv_l.at[pl.ds(0, PEERS - 1)]
    move(arrived, arrived, send_l_sem, recv_l_sem, above).wait_recv()
    for k in range(4):
        regroup(recv_l, k, store_left(k))
    sums((z, range(HELD)))
    sums(*((stream.block(1), range(HELD)) for stream in streams))
    forward(4)
    late(1, 1)
    s_far(2)
    s_far(3)
    s_late(0)
    s_far(4)
    for stream in streams:
        stream.wait(right.at[pl.ds(0, 2)], 16)
    s_far(5)
    s_late(1)

    sent = send_r.at[pl.ds(0, PEERS - 1)]
    move(sent, sent, send_r_sem, recv_r_sem.at[0], above).wait_send()
    move(sent, sent, send_l_sem, recv_l_sem, above).wait_send()
    move(sent, sent, send_x_sem, recv_x_sem, above).wait_send()
    sent = right.at[pl.ds(0, 14)]
    move(sent, sent, up_s, up_r.at[0], above).wait_send()
    move(sent, sent, down_s, down_r.at[0], below).wait_send()
    sent = s_send.at[pl.ds(0, (PEERS - 1) * 32)]
    move(sent, sent, s_s, s_r, above).wait_send()
    arrived = s_recv.at[pl.ds(0, (PEERS - 1) * 32)]
    move(arrived, arrived, s_s, s_r, above).wait_recv()
    for t in range(8):
        v = s_recv[pl.ds(t, 128, stride=8), :]
        average = jnp.mean(v, axis=0, keepdims=True)
        variance = jnp.mean(jnp.square(v - average), axis=0, keepdims=True)
        n = ((v - average) * lax.rsqrt(variance + 1e-05) * column[0] + column[1]).astype(jnp.bfloat16)
        o = dot(n, w_out[...], TN)
        out_ref[0, t] = gate[t] * o[:64]
        out_ref[1, t] = gate[t + 8] * o[64:]


def local(pair_map, pair_mask, in_gain, in_bias, w_proj, w_gate, out_gain, out_bias, w_out):
    f32, bf16 = jnp.float32, jnp.bfloat16
    vmem, dma = pltpu.VMEM, pltpu.SemaphoreType.DMA
    split = (2, 8, 64, 128)
    args = (
        pair_map.reshape(split), pair_mask, in_gain.reshape(1, -1), in_bias.reshape(1, -1), w_proj, w_gate,
        out_gain.reshape(1, -1), out_bias.reshape(1, -1), w_out,
    )
    out = pl.pallas_call(
        kernel,
        out_shape=jax.ShapeDtypeStruct(split, f32),
        in_specs=[pl.BlockSpec(memory_space=pltpu.HBM)] * 9,
        out_specs=pl.BlockSpec(memory_space=vmem),
        scratch_shapes=[
            *(vmem(a.shape, a.dtype) for a in args),
            dma, dma((8,)),
            vmem((8 * PITCH, 128), f32),
            vmem((8, 128, 128), bf16),
            vmem((16, 64, 128), f32),
            vmem((PEERS, 2, 16, 128), bf16),
            vmem((PEERS, 2, 16, 128), bf16),
            vmem((PEERS, 2, 16, 128), bf16),
            vmem((PEERS, 2, 16, 128), bf16),
            vmem((PEERS, 2, 16, 128), bf16),
            vmem((PEERS, 2, 16, 128), bf16),
            vmem((HELD, 64, 512), bf16),
            vmem((PLANES * 4, HELD, 64, 128), bf16),
            vmem((1024, 128), f32),
            vmem((1024, 128), f32),
            vmem((2, 128, 128), f32),
            dma, dma((4,)), dma, dma, dma, dma, dma, dma((20,)), dma, dma((20,)), dma, dma,
        ],
        compiler_params=pltpu.CompilerParams(
            collective_id=0, has_side_effects=True, vmem_limit_bytes=24 * 1024 * 1024
        ),
    )(*(pltpu.with_memory_space_constraint(a, pltpu.HBM) for a in args))
    return out.reshape(pair_map.shape)


def solution(mesh):
    placed = (P("row", "col", None), P("row", "col"), P(), P(), P(), P(), P(), P(), P())
    return jax.shard_map(local, mesh=mesh, in_specs=placed, out_specs=P("row", "col", None), check_vma=False)
```

```python
import jax
import jax.numpy as jnp
from jax import lax
from jax.experimental import pallas as pl
from jax.experimental.pallas import tpu as pltpu
from jax.sharding import PartitionSpec as P

MESH = pl.DeviceIdType.MESH
PLANES = 8
QUAD = 4
PEERS = 32
HELD = 4
PITCH = 136
NN = (((1,), (0,)), ((), ()))
NT = (((1,), (1,)), ((), ()))
TN = (((0,), (0,)), ((), ()))


def steps(reach):
    every = [(dx, dy, dh) for dx in range(4) for dy in range(4) for dh in range(2) if dx or dy or dh]
    return sorted(every, key=lambda s: reach(min(s[0], 4 - s[0]) + min(s[1], 4 - s[1])))


def dot(a, b, dims):
    return lax.dot_general(a, b, dims, preferred_element_type=jnp.float32)


def halves(a, b):
    low = lax.broadcasted_iota(jnp.int32, a.shape, 1) < 64
    return jnp.where(low, a, pltpu.roll(b, 64, 1)), jnp.where(low, pltpu.roll(a, 64, 1), b)


def kernel(
    x_hbm, mask_hbm, in_gain_hbm, in_bias_hbm, w_proj_hbm, w_gate_hbm, out_gain_hbm, out_bias_hbm, w_out_hbm, out_ref,
    x_ref, mask_ref, in_gain, in_bias, w_proj, w_gate, out_gain, out_bias, w_out, x_sem, in_sem,
    stage, normed, gate, send_r, send_l, recv_r, recv_l, raw, recv_x, left, right, s_send, s_recv, column,
    send_r_sem, recv_r_sem, send_l_sem, recv_l_sem, send_x_sem, recv_x_sem, up_s, up_r, down_s, down_r, s_s, s_r,
):
    row, col = lax.axis_index("row"), lax.axis_index("col")
    z, quarter = lax.div(row, QUAD), lax.rem(row, QUAD)
    me = col * QUAD + quarter
    x = lax.div(col, 4) * 2 + lax.div(quarter, 2)
    y, core = lax.rem(col, 4), lax.rem(quarter, 2)
    strip = lax.div(col, 2)
    above = {"row": lax.rem(row + QUAD, PLANES * QUAD), "col": col}
    below = {"row": lax.rem(row + (PLANES - 1) * QUAD, PLANES * QUAD), "col": col}

    def peer(other):
        return {"row": z * QUAD + lax.rem(other, QUAD), "col": lax.div(other, QUAD)}

    at_x = [lax.rem(x + n, 4) for n in range(4)]
    at_y = [lax.rem(y + n, 4) for n in range(4)]
    at_core = [core, 1 - core]
    pair_x, odd_x = [lax.div(v, 2) * 4 for v in at_x], [lax.rem(v, 2) * 2 for v in at_x]
    row_x = [z * QUAD + v for v in odd_x]
    slot_x = [4 * p + q for p, q in zip(pair_x, odd_x)]
    slot_y = [4 * v for v in at_y]

    def each(reach, step):
        for dx, dy, dh in steps(reach):
            to = {"row": row_x[dx] + at_core[dh], "col": pair_x[dx] + at_y[dy]}
            step(slot_x[dx] + slot_y[dy] + at_core[dh], to)

    x_in = pltpu.make_async_copy(x_hbm, x_ref, x_sem)
    small = [
        pltpu.make_async_copy(src, dst, in_sem.at[n])
        for n, (src, dst) in enumerate((
            (in_gain_hbm, in_gain), (in_bias_hbm, in_bias), (w_proj_hbm, w_proj), (mask_hbm, mask_ref),
            (w_gate_hbm, w_gate), (out_gain_hbm, out_gain), (out_bias_hbm, out_bias), (w_out_hbm, w_out),
        ))
    ]
    for copy in (*small[:4], x_in, *small[4:]):
        copy.start()
    barrier = pltpu.get_barrier_semaphore()
    each(lambda hops: -hops, lambda _, to: pl.semaphore_signal(barrier, inc=1, device_id=to, device_id_type=MESH))
    for neighbour in (above, below):
        pl.semaphore_signal(barrier, inc=1, device_id=neighbour, device_id_type=MESH)

    for copy in small[:4]:
        copy.wait()

    lane_low = lax.broadcasted_iota(jnp.int32, (8, 128), 1) < 64
    mask = mask_ref[...].astype(jnp.float32)
    masked = jnp.concatenate([mask[:8], mask[8:]], axis=1)
    weights = jnp.transpose(w_proj[...].astype(jnp.float32)).astype(jnp.bfloat16)

    def layer_norm_in(t):
        v = jnp.concatenate([x_ref[0, t], x_ref[1, t]], axis=0)
        average = jnp.mean(v, axis=1, keepdims=True)
        variance = jnp.mean(jnp.square(v - average), axis=1, keepdims=True)
        return ((v - average) * lax.rsqrt(variance + 1e-05) * in_gain[...] + in_bias[...]).astype(jnp.bfloat16)

    def project(t, first):
        p = dot(weights[first : first + 256], normed[t], NT)
        side = masked[t : t + 1] * jax.nn.sigmoid(p[:128]) * p[128:]
        stage[pl.ds(t * PITCH, 128), :] = side

    def pack(send):
        for g in range(64):
            pair = [stage[pl.ds(2 * g + e, 8, stride=PITCH), :] for e in range(2)]
            send[g // 2, g % 2] = jnp.concatenate(pair, axis=0).astype(jnp.bfloat16)

    def move(src, dst, send_sem, recv_sem, to):
        return pltpu.make_async_remote_copy(
            src_ref=src, dst_ref=dst, send_sem=send_sem, recv_sem=recv_sem, device_id=to, device_id_type=MESH
        )

    def regroup(recv, strip, store):
        for g in range(2):
            for rr in range(QUAD):
                a = recv[8 * strip + rr, g].astype(jnp.float32)
                b = recv[8 * strip + 4 + rr, g].astype(jnp.float32)
                first, second = halves(a, b)
                for e in range(2):
                    rows = slice(8 * e, 8 * e + 8)
                    tile = jnp.concatenate([first[rows], second[rows]], axis=0).astype(jnp.bfloat16)
                    store(2 * g + e, slice(16 * rr, 16 * rr + 16), tile)

    def near(e):
        return lax.rem(lax.div(strip, 2) + e // 2, 2) * 2 + lax.rem(strip + e % 2, 2)

    class Stream:
        def __init__(self, sign, to, far, sends, recvs):
            self.sign, self.to, self.far, self.sends, self.recvs = sign, to, far, sends, recvs
            self.rest = (2, 3) if far == 0 else (0, 1)

        def block(self, d):
            return lax.rem(z + (PLANES - d if self.sign > 0 else d), PLANES)

        def raw(self, e):
            at = pl.ds(8 * near(e), 8)
            src, dst = send_r.at[at, self.rest[0] // 2], raw.at[at, self.far // 2]
            return move(src, dst, self.sends, self.recvs.at[17], self.to)

        def strip(self, d, e):
            part = right.at[self.block(d - 1) * 4 + near(e), pl.ds(self.far, 2)]
            return move(part, part, self.sends, self.recvs.at[4 * (d - 1) + e if d < 5 else 16], self.to)

        def half(self, n, h):
            part = right.at[pl.ds(self.block(1) * 4 + 2 * h, 2), self.rest[n]]
            return move(part, part, self.sends, self.recvs.at[18 + n], self.to)

        def wait(self, part, slot):
            move(part, part, self.sends, self.recvs.at[slot], self.to).wait_recv()

    streams = (Stream(1, above, 0, up_s, up_r), Stream(-1, below, 2, down_s, down_r))

    def pass_on(e):
        for n in range(0 if e else 1, 8):
            o = 8 * near(e) + lax.rem(me + n, 8)
            move(raw.at[o], recv_x.at[me], send_x_sem, recv_x_sem, peer(o)).start()

    x_in.wait()
    for t in range(8):
        normed[t] = layer_norm_in(t)
        project(t, 256)
    pack(send_r)
    pl.semaphore_wait(barrier, PEERS - 1 + 2)
    for e in (3, 2, 1, 0):
        for stream in streams:
            stream.raw(e).start()
    each(
        lambda hops: (1, 2, 3, 4, 0)[hops],
        lambda o, to: move(send_r.at[o], recv_r.at[me], send_r_sem, recv_r_sem.at[strip], to).start(),
    )
    recv_r[me] = send_r[me]

    for t in range(8):
        project(t, 0)
    pack(send_l)
    recv_l[me] = send_l[me]

    for copy in small[4:]:
        copy.wait()
    for t in range(8):
        p = jax.nn.sigmoid(dot(normed[t], w_gate[...], NN))
        gate[t] = p[:64]
        gate[t + 8] = p[64:]
    column[0] = jnp.transpose(jnp.broadcast_to(out_gain[...], (128, 128)))
    column[1] = jnp.transpose(jnp.broadcast_to(out_bias[...], (128, 128)))

    for e in range(4):
        got = near(e)
        arrived = recv_r.at[pl.ds(8 * got, 8 if e else 7)]
        move(arrived, arrived, send_r_sem, recv_r_sem.at[got], above).wait_recv()

        def store_right(ch, rows, tile, got=got):
            right[z * 4 + got, ch, rows] = tile

        regroup(recv_r, got, store_right)
        for stream in streams:
            stream.strip(1, e).start()
        if e == 1:
            for stream in streams:
                stream.wait(raw.at[pl.ds(0, 16)], 17)
            for part in (3, 2, 1, 0):
                pass_on(part)
            recv_x[me] = raw[me]
        if e == 2:
            each(
                lambda hops: -hops,
                lambda o, to: move(send_l.at[o], recv_l.at[me], send_l_sem, recv_l_sem, to).start(),
            )

    def store_left(strip):
        def store(ch, rows, tile):
            left[ch, rows, slice(128 * strip, 128 * strip + 128)] = tile

        return store

    def sums(*parts):
        done = []
        for block, channels in parts:
            tiles = []
            for ch in channels:
                r = jnp.concatenate([right[block * 4 + k, ch] for k in range(4)], axis=1)
                s = dot(left[ch], jnp.concatenate([r, r], axis=0), NT)
                tiles.append([
                    jnp.where(lane_low, s[16 * rr : 16 * rr + 8], s[16 * rr + 8 : 16 * rr + 16]) for rr in range(QUAD)
                ])
            done.append([jnp.concatenate([t[rr] for t in tiles], axis=0) for rr in range(QUAD)])
        for (block, channels), tiles in zip(parts, done):
            first, count = channels[0] * 8, len(channels) * 8
            dst = s_recv.at[pl.ds(pl.multiple_of(me * 32 + first, 8), count)]
            for rr in range(QUAD):
                src = s_send.at[pl.ds(pl.multiple_of((block * QUAD + rr) * 32 + first, 8), count)]
                src[...] = tiles[rr]
            for rr in range(QUAD):
                src = s_send.at[pl.ds(pl.multiple_of((block * QUAD + rr) * 32 + first, 8), count)]
                mine = jnp.logical_and(block == col, quarter == rr)

                @pl.when(mine)
                def _():
                    dst[...] = src[...]

                @pl.when(jnp.logical_not(mine))
                def _():
                    move(src, dst, s_s, s_r, {"row": z * QUAD + rr, "col": block}).start()

    def forward(d, strips=range(4)):
        for e in strips:
            for stream in reversed(streams):
                stream.strip(d, e).wait_recv()
                stream.strip(d + 1, e).start()

    def late(n, h):
        for stream in streams:
            stream.half(n, h).start()

    def s_late(n):
        for stream in streams:
            stream.wait(right.at[0], 18 + n)
        sums(*((stream.block(2), (stream.rest[n],)) for stream in streams))

    def s_far(d):
        sums(*((stream.block(d), range(stream.far, stream.far + 2)) for stream in streams))

    forward(1)
    forward(2)
    forward(3, range(1))
    arrived = recv_x.at[pl.ds(0, PEERS - 1)]
    move(arrived, arrived, send_x_sem, recv_x_sem, above).wait_recv()
    for k in range(4):

        def store_next(ch, rows, tile, k=k):
            stream = streams[ch // 2]
            right[stream.block(1) * 4 + k, stream.rest[ch % 2], rows] = tile

        regroup(recv_x, k, store_next)
    late(0, 0)
    forward(3, range(1, 4))
    late(0, 1)
    late(1, 0)
    arrived = recv_l.at[pl.ds(0, PEERS - 1)]
    move(arrived, arrived, send_l_sem, recv_l_sem, above).wait_recv()
    for k in range(4):
        regroup(recv_l, k, store_left(k))
    sums((z, range(HELD)))
    sums(*((stream.block(1), range(HELD)) for stream in streams))
    forward(4)
    late(1, 1)
    s_far(2)
    s_far(3)
    s_late(0)
    s_far(4)
    for stream in streams:
        stream.wait(right.at[pl.ds(0, 2)], 16)
    s_far(5)
    s_late(1)

    sent = send_r.at[pl.ds(0, PEERS - 1)]
    move(sent, sent, send_r_sem, recv_r_sem.at[0], above).wait_send()
    move(sent, sent, send_l_sem, recv_l_sem, above).wait_send()
    move(sent, sent, send_x_sem, recv_x_sem, above).wait_send()
    sent = right.at[pl.ds(0, 14)]
    move(sent, sent, up_s, up_r.at[0], above).wait_send()
    move(sent, sent, down_s, down_r.at[0], below).wait_send()
    sent = s_send.at[pl.ds(0, (PEERS - 1) * 32)]
    move(sent, sent, s_s, s_r, above).wait_send()
    arrived = s_recv.at[pl.ds(0, (PEERS - 1) * 32)]
    move(arrived, arrived, s_s, s_r, above).wait_recv()
    for t in range(8):
        v = s_recv[pl.ds(t, 128, stride=8), :]
        average = jnp.mean(v, axis=0, keepdims=True)
        variance = jnp.mean(jnp.square(v - average), axis=0, keepdims=True)
        n = ((v - average) * lax.rsqrt(variance + 1e-05) * column[0] + column[1]).astype(jnp.bfloat16)
        o = dot(n, w_out[...], TN)
        out_ref[0, t] = gate[t] * o[:64]
        out_ref[1, t] = gate[t + 8] * o[64:]


def local(pair_map, pair_mask, in_gain, in_bias, w_proj, w_gate, out_gain, out_bias, w_out):
    f32, bf16 = jnp.float32, jnp.bfloat16
    vmem, dma = pltpu.VMEM, pltpu.SemaphoreType.DMA
    split = (2, 8, 64, 128)
    args = (
        pair_map.reshape(split), pair_mask, in_gain.reshape(1, -1), in_bias.reshape(1, -1), w_proj, w_gate,
        out_gain.reshape(1, -1), out_bias.reshape(1, -1), w_out,
    )
    out = pl.pallas_call(
        kernel,
        out_shape=jax.ShapeDtypeStruct(split, f32),
        in_specs=[pl.BlockSpec(memory_space=pltpu.HBM)] * 9,
        out_specs=pl.BlockSpec(memory_space=vmem),
        scratch_shapes=[
            *(vmem(a.shape, a.dtype) for a in args),
            dma, dma((8,)),
            vmem((8 * PITCH, 128), f32),
            vmem((8, 128, 128), bf16),
            vmem((16, 64, 128), f32),
            vmem((PEERS, 2, 16, 128), bf16),
            vmem((PEERS, 2, 16, 128), bf16),
            vmem((PEERS, 2, 16, 128), bf16),
            vmem((PEERS, 2, 16, 128), bf16),
            vmem((PEERS, 2, 16, 128), bf16),
            vmem((PEERS, 2, 16, 128), bf16),
            vmem((HELD, 64, 512), bf16),
            vmem((PLANES * 4, HELD, 64, 128), bf16),
            vmem((1024, 128), f32),
            vmem((1024, 128), f32),
            vmem((2, 128, 128), f32),
            dma, dma((4,)), dma, dma, dma, dma, dma, dma((20,)), dma, dma((20,)), dma, dma,
        ],
        compiler_params=pltpu.CompilerParams(
            collective_id=0, has_side_effects=True, vmem_limit_bytes=24 * 1024 * 1024
        ),
    )(*(pltpu.with_memory_space_constraint(a, pltpu.HBM) for a in args))
    return out.reshape(pair_map.shape)


def solution(mesh):
    placed = (P("row", "col", None), P("row", "col"), P(), P(), P(), P(), P(), P(), P())
    return jax.shard_map(local, mesh=mesh, in_specs=placed, out_specs=P("row", "col", None), check_vma=False)
```
